32 devices in a mesh: tm: 16 (over z, x, core), gz: 2 (over y).
Axes of the slice: x: 2, y: 2, z: 4, core: 2. Of those that a mesh axis runs over, the one named last changes fastest.
Arguments:
- starts: float32 [16, 8, 32, 128], P('tm', 'gz'), may hold values from -6 to 6
- cell_rates: float32 [8, 32, 128], P('gz'), may hold values from 0.3 to 1
Outputs:
- slab_ends: float32 [16, 8, 32, 128], P('tm', 'gz')
- next_starts: float32 [16, 8, 32, 128], P('tm', 'gz')
The draws below stay inside these ranges and needn't reach their ends.
All inputs are finite; a program needn't handle non-finite values.
Results may differ from the reference program's by a relative error of at most 0.0001.
Values sent between devices are 32-bit elements; how exact they have to be, the bound alone decides.
A program may use at most 64 MiB of HBM per device.

```python
import jax
import jax.numpy as jnp
from jax import lax

NX = 32
NY = 128
FINE = 4
SLABS = 16
NZ = 8


def draw_starts(key, part):
    rough = jnp.clip(jax.random.normal(key, (SLABS, NZ, NX, NY), jnp.float32), -6.0, 6.0)
    return rough


def block_levels(own_key, extent, pieces, low, largest):
    def one(position, blocks):
        draws = jax.random.uniform(jax.random.fold_in(jax.random.fold_in(own_key, 6), position), (blocks,), jnp.float32, low / len(pieces), largest / len(pieces))
        return jnp.repeat(jnp.exp(draws), extent[position] // blocks).reshape((-1,) + (1,) * (len(extent) - position - 1))

    factor_of = one(*pieces[0])
    for cut in pieces[1:]:
        factor_of = factor_of * one(*cut)
    return factor_of


def setup_inputs(seed: int = 0) -> dict:
    keys = jax.random.split(jax.random.key(seed), 3)
    starts = draw_starts(jax.random.fold_in(keys[2], 71), 0)
    cell_rates = jnp.clip(0.3 + 0.7 * jax.random.uniform(keys[1], (NZ, NX, NY), jnp.float32) ** block_levels(keys[1], (NZ, NX, NY), ((0, 2),), -0.2, 0.2), 0.3, 1.0)
    return dict(starts=starts, cell_rates=cell_rates)


fine_along_z = (0.1, 0.12)
fine_along_x = (0.15, 0.12)
fine_along_y = (0.2, 0.12)
coarse_along_z = (0.2, 0.25)
coarse_along_x = (0.3, 0.25)
coarse_along_y = (0.4, 0.25)


def line_filter(behind, middle, beyond, courant, diffuse):
    return (diffuse + 0.5 * courant) * behind + (1.0 - 2.0 * diffuse) * middle + (diffuse - 0.5 * courant) * beyond


def smooth_step(values, weights, along_z, along_x, along_y):
    mixed = line_filter(jnp.roll(values, 1, 2), values, jnp.roll(values, -1, 2), along_y[0], along_y[1])
    mixed = line_filter(jnp.roll(mixed, 1, 1), mixed, jnp.roll(mixed, -1, 1), along_x[0], along_x[1])
    mixed = line_filter(jnp.roll(mixed, 1, 0), mixed, jnp.roll(mixed, -1, 0), along_z[0], along_z[1])
    return values + weights * (mixed - values)


def restrict(values):
    extent_z, extent_x, extent_y = values.shape
    blocks = values.reshape(extent_z // 2, 2, extent_x // 2, 2, extent_y // 2, 2)
    return jnp.mean(blocks, axis=(1, 3, 5))


def prolong(values):
    extent_z, extent_x, extent_y = values.shape
    spread = jnp.broadcast_to(values[:, None, :, None, :, None], (extent_z, 2, extent_x, 2, extent_y, 2))
    return spread.reshape(extent_z * 2, extent_x * 2, extent_y * 2)


def propagate(values, coarse_rates):
    coarse = smooth_step(restrict(values), coarse_rates, coarse_along_z, coarse_along_x, coarse_along_y)
    return prolong(coarse)


def fine_solve(values, cell_rates):
    for sweep_index in range(FINE):
        values = smooth_step(values, cell_rates, fine_along_z, fine_along_x, fine_along_y)
    return values


def reference(starts, cell_rates):
    coarse_rates = restrict(cell_rates)

    def slab_correction(start):
        return fine_solve(start, cell_rates) - propagate(start, coarse_rates)

    correction = lax.map(slab_correction, starts)

    def link(current, term):
        finish = propagate(current, coarse_rates) + term
        return finish, finish

    _, slab_ends = lax.scan(link, starts[0], correction)
    next_starts = jnp.concatenate([slab_ends[-1:], slab_ends[:-1]], axis=0)
    return slab_ends, next_starts
```

```python
import functools

import jax
import jax.numpy as jnp
from jax import lax
from jax.experimental import pallas as pl
from jax.experimental.pallas import tpu as pltpu
from jax.sharding import PartitionSpec as P

MESH = pl.DeviceIdType.MESH
FINE = 4

fine_along_z = (0.1, 0.12)
fine_along_x = (0.15, 0.12)
fine_along_y = (0.2, 0.12)
coarse_along_z = (0.2, 0.25)
coarse_along_x = (0.3, 0.25)
coarse_along_y = (0.4, 0.25)


def blend(behind, middle, beyond, along):
    courant, diffuse = along
    center = 1.0 - 2.0 * diffuse
    before, after = (diffuse + 0.5 * courant) / center, (diffuse - 0.5 * courant) / center
    if middle is None:
        return before * behind if beyond is None else after * beyond
    if behind is None:
        return middle if beyond is None else middle + after * beyond
    if beyond is None:
        return middle + before * behind
    return middle + (before * behind + after * beyond)


def centers(*alongs):
    product = 1.0
    for _, diffuse in alongs:
        product *= 1.0 - 2.0 * diffuse
    return product


def turned(values, by, dim):
    return pltpu.roll(values, by % values.shape[dim], dim)


def filtered(values, by, dim, along):
    return blend(turned(values, by, dim), values, turned(values, -by, dim), along)


def kernel(
    slabs, parts, starts_ref, rates_ref, end_ref, next_ref,
    state, rates, pull, keep, mixed, field, shares, shares_in, sums, wraps, crown, crown_in,
    heads, heads_in, corr_in, parts_in,
    load_sem, ready_sem, raw_sem, rate_send, rate_recv, hand_send, hand_recv, side_send, side_recv,
    next_send, next_recv, wrap_send, wrap_recv, share_send, share_recv, sum_send, sum_recv,
    part_send, part_recv, corr_sem, head_sem, crown_send, crown_recv,
):
    depth, rows, lanes = rates_ref.shape
    layers = depth * parts
    groups = slabs // 2
    coarse_layers, coarse_rows, coarse_depth = layers // 2, rows // 2, depth // 2
    half = coarse_layers // 2
    me, part = lax.axis_index("tm"), lax.axis_index("gz")
    group, place = me // 2, lax.rem(me, 2)
    leads, helps = place == 1, place == 0
    last = group == groups - 1

    def block(r):
        return pl.ds(r % parts * depth, depth)

    own = block(0)
    rate_load = pltpu.make_async_copy(rates_ref, rates.at[own], load_sem.at[1])
    state_load = pltpu.make_async_copy(starts_ref.at[0], state.at[place, own], load_sem.at[0])
    rate_load.start()
    state_load.start()

    def leader(g, i):
        return {"tm": 2 * g + 1, "gz": lax.rem(part + i, parts)}

    def helper(g, i):
        return {"tm": 2 * g, "gz": lax.rem(part + i, parts)}

    def signal(sem, peer):
        pl.semaphore_signal(sem, inc=1, device_id=peer, device_id_type=MESH)

    def remote(src, dst, send_sem, recv_sem, peer):
        return pltpu.make_async_remote_copy(
            src_ref=src, dst_ref=dst, send_sem=send_sem, recv_sem=recv_sem,
            device_id=peer, device_id_type=MESH,
        )

    others = range(1, parts)
    barrier = pltpu.get_barrier_semaphore()
    here, far, across = ready_sem.at[0], ready_sem.at[1], ready_sem.at[2]

    @pl.when(leads)
    def _():
        for i in others:
            signal(barrier, leader(group, i))
        signal(barrier, helper(group, 0))
        for j in range(1, groups):
            @pl.when(group + j < groups)
            def _():
                signal(barrier, leader(group + j, 0))

    @pl.when(helps)
    def _():
        for i in others:
            signal(barrier, helper(group, i))

        @pl.when(group == 0)
        def _():
            for j in range(1, groups):
                for i in range(parts):
                    signal(barrier, leader(j, i))

    earlier = group + jnp.where(group > 0, parts, 0)
    pl.semaphore_wait(barrier, jnp.where(leads, parts - 1 + earlier, parts))

    def raw_copy():
        piece = state.at[0, own]
        return remote(piece, piece, raw_sem.at[0], raw_sem.at[1], leader(group, 0))

    order = sorted(range(depth), key=lambda k: min(k, depth - 1 - k))

    def rate_copy(i, k):
        return remote(
            rates.at[k], rates.at[(parts - i) * depth + k],
            rate_send.at[i - 1, k], rate_recv.at[parts - i - 1, k], leader(group, i),
        )

    def hand_copy(i):
        piece = rates.at[block(i)]
        return remote(piece, piece, hand_send.at[i - 1], hand_recv.at[i - 1], helper(group, 0))

    def side_copy(i):
        return remote(
            state.at[0, own], state.at[0, block(parts - i)],
            side_send.at[i - 1], side_recv.at[parts - i - 1], helper(group, i),
        )

    def next_copy(i):
        return remote(
            state.at[1, own], state.at[1, block(parts - i)],
            next_send.at[i], next_recv.at[(parts - i) % parts], helper(lax.rem(group + 1, groups), i),
        )

    def wrap_copy(i):
        r = (parts - i) % parts
        return remote(
            shares.at[i, 0], wraps.at[group, r], wrap_send.at[i], wrap_recv.at[group, r], helper(0, i)
        )

    def crown_copy(i):
        r = (parts - i) % parts
        return remote(crown.at[i], crown_in.at[r], crown_send.at[i], crown_recv.at[r], helper(0, i))

    def share_copy(i):
        r = parts - i - 1
        return remote(
            shares.at[i], shares_in.at[r], share_send.at[i - 1], share_recv.at[r], leader(group, i)
        )

    def sum_copy(j):
        piece = sums.at[group]
        return remote(piece, piece, sum_send.at[j - 1], sum_recv.at[group], leader(group + j, 0))

    def part_copy(i):
        r = parts - i - 1
        return remote(
            field.at[1, block(i)], parts_in.at[r], part_send.at[i - 1], part_recv.at[r], leader(group, i)
        )

    def corr_copy():
        return remote(field.at[0, own], corr_in, corr_sem.at[0], corr_sem.at[1], leader(group, 0))

    def head_copy():
        return remote(heads, heads_in, head_sem.at[0], head_sem.at[1], helper(group, 0))

    even = lax.rem(lax.broadcasted_iota(jnp.int32, (coarse_rows, lanes), 1), 2) == 0
    sides = [pl.ds(0, coarse_rows, stride=2), pl.ds(1, coarse_rows, stride=2)]
    fine_center = centers(fine_along_y, fine_along_x, fine_along_z)
    coarse_center = centers(coarse_along_y, coarse_along_x, coarse_along_z)

    def prepare(ks):
        for k in ks:
            pull[k] = rates[k] * fine_center
            keep[k] = 1.0 - rates[k]

    def restricted(ref, layer, lead=()):
        total = (ref[(*lead, layer, sides[0])] + ref[(*lead, layer, sides[1])]) + (
            ref[(*lead, layer + 1, sides[0])] + ref[(*lead, layer + 1, sides[1])]
        )
        pair_sum = total + jnp.where(even, turned(total, -1, 1), turned(total, 1, 1))
        return pair_sum * 0.125

    def coarse_rates():
        weights = [restricted(rates, 2 * k) for k in range(coarse_layers)]
        return [w * coarse_center for w in weights], [1.0 - w for w in weights]

    def plane_filtered(values, along):
        return filtered(values, 1, 0, along)

    def advance(coarse, pulls, keeps, wanted):
        plane = [
            None if c is None else plane_filtered(filtered(c, 2, 1, coarse_along_y), coarse_along_x)
            for c in coarse
        ]
        moved = [None] * coarse_layers
        for k in wanted:
            trio = plane[k - 1], plane[k], plane[(k + 1) % coarse_layers]
            if any(p is not None for p in trio):
                moved[k] = pulls[k] * across_z(trio, coarse_along_z)
                if coarse[k] is not None:
                    moved[k] = moved[k] + keeps[k] * coarse[k]
        return moved

    def across_z(trio, along):
        behind, middle, beyond = trio
        if middle is None and behind is not None and beyond is not None:
            return blend(behind, None, None, along) + blend(None, None, beyond, along)
        return blend(behind, middle, beyond, along)

    def packed(coarse, shift=0):
        def layer(k):
            return coarse[(k + shift) % coarse_layers]

        return [jnp.where(even, layer(k), layer(k + half)) for k in range(half)]

    def shifted(c):
        return {n: turned(c, n, 1) for n in (1, 2, 3, -1, -2, -3)} | {0: c}

    def mixed_lanes(t, even_by, odd_by):
        trio = [
            t[even_by + n] if even_by == odd_by else jnp.where(even, t[even_by + n], t[odd_by + n])
            for n in (2, 0, -2)
        ]
        return trio[1], plane_filtered(blend(*trio, coarse_along_y), coarse_along_x)

    def advance_packed(coarse, pulls, keeps):
        turns = [shifted(c) for c in coarse]
        plane = [mixed_lanes(t, 0, 0)[1] for t in turns]
        low, high = mixed_lanes(turns[-1], -1, 1)[1], mixed_lanes(turns[0], -1, 1)[1]
        ring = [low] + plane + [high]
        return [
            pulls[k] * blend(ring[k], ring[k + 1], ring[k + 2], coarse_along_z) + keeps[k] * coarse[k]
            for k in range(half)
        ]

    def advance_opened(coarse, pulls, keeps):
        turns = [shifted(c) for c in coarse]

        def opened(k):
            k = k % coarse_layers
            return mixed_lanes(turns[k % half], *((0, 1) if k < half else (-1, 0)))

        ring = [opened(k) for k in range(-1, coarse_depth + 1)]
        return [
            pulls[k] * blend(ring[k][1], ring[k + 1][1], ring[k + 2][1], coarse_along_z)
            + keeps[k] * ring[k + 1][0]
            for k in range(coarse_depth)
        ]

    def plus(first, second):
        return [b if a is None else a if b is None else a + b for a, b in zip(first, second)]

    def grown(ks):
        return sorted({(k + n) % layers for k in ks for n in (-1, 0, 1)})

    def spread(s, turn, ks):
        held = state if turn == 0 else field
        for k in ks:
            mixed[s, k] = plane_filtered(filtered(held[s, k], 1, 1, fine_along_y), fine_along_x)

    def settle(s, turn, live, ks):
        held = state if turn == 0 else field
        for k in ks:
            trio = [mixed[s, n % layers] if n % layers in live else None for n in (k - 1, k, k + 1)]
            value = pull[k] * across_z(trio, fine_along_z)
            field[s, k] = value + keep[k] * held[s, k] if k in live else value

    own_layers, own_coarse = list(range(depth)), list(range(coarse_depth))
    all_layers, all_coarse = list(range(layers)), list(range(coarse_layers))
    nothing = jnp.zeros((coarse_rows, lanes), jnp.float32)

    def sent_on(s, guess, ks):
        for k in ks:
            if guess[k // 2] is not None:
                for side in sides:
                    field[s, k, side, :] = field[s, k, side, :] - guess[k // 2]

    @pl.when(leads)
    def _():
        rate_load.wait()
        for k in order:
            for i in others:
                rate_copy(i, k).start()
        state_load.wait()

        @pl.when(last)
        def _():
            for i in range(parts):
                next_copy(i).start()

        prepare(own_layers)
        spread(1, 0, own_layers)
        pl.semaphore_wait(here, 1)
        for j in range(1, groups):
            @pl.when(group - j >= 0)
            def _():
                signal(far, leader(group - j, 0))

        raw_copy().wait_recv()
        spread(0, 0, own_layers)
        edges, inner = order[:2], order[2:]
        for k in edges:
            for i in others:
                rate_copy(i, k).wait_recv()
        near = [r * depth + k for r in others for k in edges]
        prepare(near)
        live, reach = own_layers, grown(own_layers)
        for s in (1, 0):
            settle(s, 0, live, reach)
        for k in inner:
            for i in others:
                rate_copy(i, k).wait_recv()
        for i in others:
            hand_copy(i).start()
        prepare([k for k in all_layers if k not in own_layers + near])
        pulls, keeps = coarse_rates()
        guesses = []
        for s, gate in ((0, jnp.where(group > 0, 1.0, 0.0)), (1, None)):
            begin = [restricted(state, 2 * k, (s,)) for k in own_coarse]
            begin = begin + [None] * (coarse_layers - coarse_depth)
            guess = advance(begin, pulls, keeps, all_coarse)
            guesses.append([g if g is None or gate is None else gate * g for g in guess])
        for turn in range(1, FINE):
            live, reach = reach, grown(reach)
            for s in (0, 1):
                spread(s, turn, live)
            for s in (0, 1):
                settle(s, turn, live, reach)
        live = reach
        for s in (0, 1):
            for k in all_layers:
                if k not in live:
                    field[s, k] = jnp.zeros((rows, lanes), jnp.float32)

        def term_of(s):
            return [
                None
                if 2 * k not in live and guesses[s][k] is None
                else restricted(field, 2 * k, (s,))
                - (nothing if guesses[s][k] is None else guesses[s][k])
                for k in all_coarse
            ]

        term, after = term_of(0), term_of(1)
        run = plus(advance(term, pulls, keeps, all_coarse), after)
        run, term = ([nothing if t is None else t for t in x] for x in (run, term))
        for i in range(parts):
            shift = i * coarse_depth
            for k, c in enumerate(packed(run, shift)):
                shares[i, 0, k] = c
            for k, c in enumerate(packed(term, shift)):
                shares[i, 1, k] = c
            for k in own_coarse:
                crown[i, k] = run[(k + shift) % coarse_layers]

        @pl.when(last)
        def _():
            for i in range(parts):
                crown_copy(i).start()

        @pl.when(~last & (group > 0))
        def _():
            for i in range(parts):
                wrap_copy(i).start()

        for i in others:
            share_copy(i).start()
        sent_on(1, guesses[1], all_layers)
        @pl.when(~last)
        def _():
            pl.semaphore_wait(far, groups - 1 - group)

        for i in others:
            signal(across, leader(group, i))
        total, middle = packed(run), packed(term)
        for r in others:
            share_copy(parts - r).wait_recv()
            total = plus(total, [shares_in[r - 1, 0, k] for k in range(half)])
            middle = plus(middle, [shares_in[r - 1, 1, k] for k in range(half)])
        for k in range(half):
            sums[group, k] = total[k]
        for j in reversed(range(1, groups)):
            @pl.when(group + j < groups)
            def _():
                sum_copy(j).start()

        if parts > 1:
            pl.semaphore_wait(across, parts - 1)

        @pl.when(group == 0)
        def _():
            for i in range(parts):
                wrap_copy(i).start()

        @pl.when(~last)
        def _():
            for i in range(parts):
                next_copy(i).start()

        for i in others:
            part_copy(i).start()

        packed_pulls, packed_keeps = packed(pulls), packed(keeps)

        def take(index):
            piece = sums.at[index]
            remote(piece, piece, sum_send.at[0], sum_recv.at[index], leader(group, 1)).wait_recv()

        @pl.when(group > 0)
        def _():
            take(0)

        begun = jnp.where(group > 0, 1.0, 0.0)
        coarse = tuple(begun * sums[0, k] for k in range(half))

        def pass_group(index, coarse):
            for _ in range(2):
                coarse = advance_packed(coarse, packed_pulls, packed_keeps)
            take(index)
            return tuple(plus(coarse, [sums[index, k] for k in range(half)]))

        coarse = list(lax.fori_loop(1, jnp.maximum(group, 1), pass_group, coarse))
        ahead = advance_opened(coarse, pulls, keeps)
        opened = []
        for k in own_coarse:
            both = coarse[k % half]
            opened.append(
                jnp.where(even, both, turned(both, 1, 1))
                if k < half
                else jnp.where(even, turned(both, -1, 1), both)
            )
        for k in own_coarse:
            heads[0, k] = opened[k]
            heads[1, k] = ahead[k]

        @pl.when(group > 0)
        def _():
            head_copy().start()

        finish = advance_opened(
            plus(advance_packed(coarse, packed_pulls, packed_keeps), middle), pulls, keeps
        )
        corr_copy().wait_recv()
        for r in others:
            part_copy(parts - r).wait_recv()
        for k in own_layers:
            for side in sides:
                next_ref[0, k, side, :] = corr_in[k, side, :] + ahead[k // 2]
                held = field[1, k, side, :]
                for r in others:
                    held = held + parts_in[r - 1, k, side, :]
                end_ref[0, k, side, :] = held + finish[k // 2]
        for i in others:
            for k in order:
                rate_copy(i, k).wait_send()
            hand_copy(i).wait_send()
            share_copy(i).wait_send()
            part_copy(i).wait_send()
        for i in range(parts):
            next_copy(i).wait_send()
        for j in range(1, groups):
            @pl.when(group + j < groups)
            def _():
                sum_copy(j).wait_send()

        @pl.when(last)
        def _():
            for i in range(parts):
                crown_copy(i).wait_send()

        @pl.when(~last)
        def _():
            for i in range(parts):
                wrap_copy(i).wait_send()

        @pl.when(group > 0)
        def _():
            head_copy().wait_send()

    @pl.when(helps)
    def _():
        signal(here, leader(group, 0))
        state_load.wait()
        raw_copy().start()
        rate_load.wait()
        prepare(own_layers)
        raw_copy().wait_send()
        for i in others:
            side_copy(i).start()
        for i in others:
            side_copy(i).wait_recv()
            hand_copy(i).wait_recv()
        prepare([k for k in all_layers if k not in own_layers])
        pulls, keeps = coarse_rates()

        def solve(s, gate):
            begin = [restricted(state, 2 * k, (s,)) for k in all_coarse]
            guess = advance(begin, pulls, keeps, own_coarse)
            if gate is not None:
                guess = [g if g is None else gate * g for g in guess]
            wanted = [own_layers]
            for _ in range(1, FINE):
                wanted.append(grown(wanted[-1]))
            for turn in range(FINE):
                reach = wanted[FINE - 1 - turn]
                spread(s, turn, grown(reach))
                settle(s, turn, all_layers, reach)
            sent_on(s, guess, own_layers)

        solve(0, jnp.where(group > 0, 1.0, 0.0))
        corr_copy().start()
        for r in range(parts):
            next_copy(r).wait_recv()
        solve(1, None)
        before = [restricted(field, 2 * k, (1,)) for k in own_coarse]
        for k in own_layers:
            for side in sides:
                next_ref[0, k, side, :] = field[1, k, side, :] - before[k // 2]
                end_ref[0, k, side, :] = field[0, k, side, :]

        @pl.when(group == 0)
        def _():
            packed_pulls, packed_keeps = packed(pulls), packed(keeps)

            def pass_group(index, coarse):
                for _ in range(2):
                    coarse = advance_packed(coarse, packed_pulls, packed_keeps)
                for r in range(parts):
                    piece = wraps.at[index, r]
                    remote(
                        piece, piece, wrap_send.at[0], wrap_recv.at[index, r], leader(0, 0)
                    ).wait_recv()
                    coarse = plus(coarse, [wraps[index, r, k] for k in range(half)])
                return tuple(coarse)

            coarse = list(lax.fori_loop(0, groups - 1, pass_group, (nothing,) * half))
            coarse = advance_packed(coarse, packed_pulls, packed_keeps)
            coarse = advance_opened(coarse, pulls, keeps)
            for k in own_layers:
                for side in sides:
                    next_ref[0, k, side, :] = next_ref[0, k, side, :] + coarse[k // 2]
            for r in range(parts):
                crown_copy((parts - r) % parts).wait_recv()
            for k in own_layers:
                offset = crown_in[0, k // 2]
                for r in others:
                    offset = offset + crown_in[r, k // 2]
                for side in sides:
                    next_ref[0, k, side, :] = next_ref[0, k, side, :] + offset

        @pl.when(group > 0)
        def _():
            head_copy().wait_recv()
            for k in own_layers:
                for side in sides:
                    next_ref[0, k, side, :] = next_ref[0, k, side, :] + heads_in[0, k // 2]
                    end_ref[0, k, side, :] = end_ref[0, k, side, :] + heads_in[1, k // 2]

        corr_copy().wait_send()
        for i in others:
            side_copy(i).wait_send()


def hand_out_kernel(end_ref, next_ref, end_out, next_out, sems):
    copies = [
        pltpu.make_async_copy(end_ref, end_out, sems.at[0]),
        pltpu.make_async_copy(next_ref, next_out, sems.at[1]),
    ]
    for copy in copies:
        copy.start()
    for copy in copies:
        copy.wait()


def hand_out(end, following):
    return pl.pallas_call(
        hand_out_kernel,
        out_shape=[jax.ShapeDtypeStruct(end.shape, end.dtype)] * 2,
        in_specs=[pl.BlockSpec(memory_space=pltpu.VMEM)] * 2,
        out_specs=[pl.BlockSpec(memory_space=pl.ANY)] * 2,
        scratch_shapes=[pltpu.SemaphoreType.DMA((2,))],
    )(*(pltpu.with_memory_space_constraint(x, pltpu.VMEM) for x in (end, following)))


def solution(mesh):
    slabs, parts = mesh.shape["tm"], mesh.shape["gz"]

    def per_device(starts, cell_rates):
        depth, rows, lanes = cell_rates.shape
        layers = depth * parts
        groups = slabs // 2
        packed = (layers // 4, rows // 2, lanes)
        lead = (depth // 2, rows // 2, lanes)
        aside = max(parts - 1, 1)
        dma = pltpu.SemaphoreType.DMA

        def vmem(*shape):
            return pltpu.VMEM(shape, jnp.float32)

        ends = pl.pallas_call(
            functools.partial(kernel, slabs, parts),
            out_shape=[pltpu.VMEM(starts.shape, jnp.float32)] * 2,
            in_specs=[pl.BlockSpec(memory_space=pl.ANY)] * 2,
            out_specs=[pl.BlockSpec(memory_space=pltpu.VMEM)] * 2,
            scratch_shapes=[
                vmem(2, layers, rows, lanes),
                vmem(layers, rows, lanes),
                vmem(layers, rows, lanes),
                vmem(layers, rows, lanes),
                vmem(2, layers, rows, lanes),
                vmem(2, layers, rows, lanes),
                vmem(parts, 2, *packed),
                vmem(aside, 2, *packed),
                vmem(groups, *packed),
                vmem(groups, parts, *packed),
                vmem(parts, *lead),
                vmem(parts, *lead),
                vmem(2, *lead),
                vmem(2, *lead),
                vmem(depth, rows, lanes),
                vmem(aside, depth, rows, lanes),
                dma((2,)),
                pltpu.SemaphoreType.REGULAR((3,)),
                dma((2,)),
            ]
            + [dma((aside, depth))] * 2
            + [dma((aside,))] * 4
            + [dma((parts,))] * 2
            + [dma((parts,)), dma((groups, parts))]
            + [dma((aside,))] * 2
            + [dma((max(groups - 1, 1),)), dma((groups,))]
            + [dma((aside,))] * 2
            + [dma((2,))] * 2
            + [dma((parts,))] * 2,
            compiler_params=pltpu.CompilerParams(collective_id=0, has_side_effects=True),
        )(starts, cell_rates)
        return hand_out(*ends)

    return jax.shard_map(
        per_device,
        mesh=mesh,
        in_specs=(P("tm", "gz", None, None), P("gz", None, None)),
        out_specs=(P("tm", "gz", None, None), P("tm", "gz", None, None)),
        check_vma=False,
    )
```

```python
import functools

import jax
import jax.numpy as jnp
from jax import lax
from jax.experimental import pallas as pl
from jax.experimental.pallas import tpu as pltpu
from jax.sharding import PartitionSpec as P

MESH = pl.DeviceIdType.MESH
FINE = 4

fine_along_z = (0.1, 0.12)
fine_along_x = (0.15, 0.12)
fine_along_y = (0.2, 0.12)
coarse_along_z = (0.2, 0.25)
coarse_along_x = (0.3, 0.25)
coarse_along_y = (0.4, 0.25)


def blend(behind, middle, beyond, along):
    courant, diffuse = along
    center = 1.0 - 2.0 * diffuse
    before, after = (diffuse + 0.5 * courant) / center, (diffuse - 0.5 * courant) / center
    if middle is None:
        return before * behind if beyond is None else after * beyond
    if behind is None:
        return middle if beyond is None else middle + after * beyond
    if beyond is None:
        return middle + before * behind
    return middle + (before * behind + after * beyond)


def centers(*alongs):
    product = 1.0
    for _, diffuse in alongs:
        product *= 1.0 - 2.0 * diffuse
    return product


def turned(values, by, dim):
    return pltpu.roll(values, by % values.shape[dim], dim)


def filtered(values, by, dim, along):
    return blend(turned(values, by, dim), values, turned(values, -by, dim), along)


def kernel(
    slabs, parts, starts_ref, rates_ref, end_ref, next_ref,
    state, rates, pull, keep, mixed, field, shares, shares_in, sums, wraps, crown, crown_in,
    heads, heads_in, corr_in, parts_in,
    ready, leave, arrive,
):
    depth, rows, lanes = rates_ref.shape
    layers = depth * parts
    groups = slabs // 2
    coarse_layers, coarse_rows, coarse_depth = layers // 2, rows // 2, depth // 2
    half = coarse_layers // 2
    me, part = lax.axis_index("tm"), lax.axis_index("gz")
    group, place = me // 2, lax.rem(me, 2)
    leads, helps = place == 1, place == 0
    last = group == groups - 1

    def block(r):
        return pl.ds(r % parts * depth, depth)

    own = block(0)
    rate_load = pltpu.make_async_copy(rates_ref, rates.at[own], leave.at[5])
    state_load = pltpu.make_async_copy(starts_ref.at[0], state.at[place, own], leave.at[6])
    rate_load.start()
    state_load.start()

    def leader(g, i):
        return {"tm": 2 * g + 1, "gz": lax.rem(part + i, parts)}

    def helper(g, i):
        return {"tm": 2 * g, "gz": lax.rem(part + i, parts)}

    def signal(sem, peer):
        pl.semaphore_signal(sem, inc=1, device_id=peer, device_id_type=MESH)

    def remote(src, dst, send_sem, recv_sem, peer):
        return pltpu.make_async_remote_copy(
            src_ref=src, dst_ref=dst, send_sem=send_sem, recv_sem=recv_sem,
            device_id=peer, device_id_type=MESH,
        )

    others = range(1, parts)
    barrier = pltpu.get_barrier_semaphore()
    here, near_open, far_open, across = (ready.at[n] for n in range(4))
    line = 6

    @pl.when(leads)
    def _():
        for i in others:
            signal(barrier, leader(group, i))
        signal(barrier, helper(group, 0))
        for j in range(1, groups):
            @pl.when(group + j < groups)
            def _():
                signal(barrier, leader(group + j, 0))

    @pl.when(helps)
    def _():
        for i in others:
            signal(barrier, helper(group, i))

        @pl.when(group == 0)
        def _():
            for j in range(1, groups):
                for i in range(parts):
                    signal(barrier, leader(j, i))

    earlier = group + jnp.where(group > 0, parts, 0)
    pl.semaphore_wait(barrier, jnp.where(leads, parts - 1 + earlier, parts))

    def drain(sem, ref):
        pltpu.make_async_copy(ref, ref, sem).wait()

    def raw_copy():
        piece = state.at[0, own]
        return remote(piece, piece, leave.at[0], arrive.at[0], leader(group, 0))

    order = sorted(range(depth), key=lambda k: min(k, depth - 1 - k))
    edges, inner = order[:2], order[2:]

    def rate_copy(i, k):
        return remote(
            rates.at[k], rates.at[(parts - i) * depth + k],
            leave.at[0], arrive.at[1 if k in edges else 2], leader(group, i),
        )

    def hand_copy(i):
        piece = rates.at[block(i)]
        return remote(piece, piece, leave.at[1], arrive.at[1], helper(group, 0))

    def side_copy(i):
        return remote(
            state.at[0, own], state.at[0, block(parts - i)], leave.at[1], arrive.at[2], helper(group, i)
        )

    def next_copy(i):
        return remote(
            state.at[1, own], state.at[1, block(parts - i)], leave.at[2], arrive.at[0],
            helper(lax.rem(group + 1, groups), i),
        )

    def wrap_copy(i):
        return remote(
            shares.at[i, 0], wraps.at[group, (parts - i) % parts], leave.at[3], arrive.at[line + group],
            helper(0, i),
        )

    def crown_copy(i):
        return remote(
            crown.at[i], crown_in.at[(parts - i) % parts], leave.at[3], arrive.at[line + group],
            helper(0, i),
        )

    def share_copy(i):
        return remote(shares.at[i], shares_in.at[parts - i - 1], leave.at[4], arrive.at[3], leader(group, i))

    def sum_copy(j):
        piece = sums.at[group]
        return remote(piece, piece, leave.at[7], arrive.at[line + group], leader(group + j, 0))

    def part_copy(i):
        return remote(
            field.at[1, block(i)], parts_in.at[parts - i - 1], leave.at[5], arrive.at[4], leader(group, i)
        )

    def corr_copy():
        return remote(field.at[0, own], corr_in, leave.at[2], arrive.at[5], leader(group, 0))

    def head_copy():
        return remote(heads, heads_in, leave.at[6], arrive.at[3], helper(group, 0))

    even = lax.rem(lax.broadcasted_iota(jnp.int32, (coarse_rows, lanes), 1), 2) == 0
    sides = [pl.ds(0, coarse_rows, stride=2), pl.ds(1, coarse_rows, stride=2)]
    fine_center = centers(fine_along_y, fine_along_x, fine_along_z)
    coarse_center = centers(coarse_along_y, coarse_along_x, coarse_along_z)

    def prepare(ks):
        for k in ks:
            pull[k] = rates[k] * fine_center
            keep[k] = 1.0 - rates[k]

    def restricted(ref, layer, lead=()):
        total = (ref[(*lead, layer, sides[0])] + ref[(*lead, layer, sides[1])]) + (
            ref[(*lead, layer + 1, sides[0])] + ref[(*lead, layer + 1, sides[1])]
        )
        pair_sum = total + jnp.where(even, turned(total, -1, 1), turned(total, 1, 1))
        return pair_sum * 0.125

    def coarse_rates():
        weights = [restricted(rates, 2 * k) for k in range(coarse_layers)]
        return [w * coarse_center for w in weights], [1.0 - w for w in weights]

    def plane_filtered(values, along):
        return filtered(values, 1, 0, along)

    def advance(coarse, pulls, keeps, wanted):
        plane = [
            None if c is None else plane_filtered(filtered(c, 2, 1, coarse_along_y), coarse_along_x)
            for c in coarse
        ]
        moved = [None] * coarse_layers
        for k in wanted:
            trio = plane[k - 1], plane[k], plane[(k + 1) % coarse_layers]
            if any(p is not None for p in trio):
                moved[k] = pulls[k] * across_z(trio, coarse_along_z)
                if coarse[k] is not None:
                    moved[k] = moved[k] + keeps[k] * coarse[k]
        return moved

    def across_z(trio, along):
        behind, middle, beyond = trio
        if middle is None and behind is not None and beyond is not None:
            return blend(behind, None, None, along) + blend(None, None, beyond, along)
        return blend(behind, middle, beyond, along)

    def packed(coarse, shift=0):
        def layer(k):
            return coarse[(k + shift) % coarse_layers]

        return [jnp.where(even, layer(k), layer(k + half)) for k in range(half)]

    def shifted(c):
        return {n: turned(c, n, 1) for n in (1, 2, 3, -1, -2, -3)} | {0: c}

    def mixed_lanes(t, even_by, odd_by):
        trio = [
            t[even_by + n] if even_by == odd_by else jnp.where(even, t[even_by + n], t[odd_by + n])
            for n in (2, 0, -2)
        ]
        return trio[1], plane_filtered(blend(*trio, coarse_along_y), coarse_along_x)

    def advance_packed(coarse, pulls, keeps):
        turns = [shifted(c) for c in coarse]
        plane = [mixed_lanes(t, 0, 0)[1] for t in turns]
        low, high = mixed_lanes(turns[-1], -1, 1)[1], mixed_lanes(turns[0], -1, 1)[1]
        ring = [low] + plane + [high]
        return [
            pulls[k] * blend(ring[k], ring[k + 1], ring[k + 2], coarse_along_z) + keeps[k] * coarse[k]
            for k in range(half)
        ]

    def advance_opened(coarse, pulls, keeps):
        turns = [shifted(c) for c in coarse]

        def opened(k):
            k = k % coarse_layers
            return mixed_lanes(turns[k % half], *((0, 1) if k < half else (-1, 0)))

        ring = [opened(k) for k in range(-1, coarse_depth + 1)]
        return [
            pulls[k] * blend(ring[k][1], ring[k + 1][1], ring[k + 2][1], coarse_along_z)
            + keeps[k] * ring[k + 1][0]
            for k in range(coarse_depth)
        ]

    def plus(first, second):
        return [b if a is None else a if b is None else a + b for a, b in zip(first, second)]

    def grown(ks):
        return sorted({(k + n) % layers for k in ks for n in (-1, 0, 1)})

    def spread(s, turn, ks):
        held = state if turn == 0 else field
        for k in ks:
            mixed[s, k] = plane_filtered(filtered(held[s, k], 1, 1, fine_along_y), fine_along_x)

    def settle(s, turn, live, ks):
        held = state if turn == 0 else field
        for k in ks:
            trio = [mixed[s, n % layers] if n % layers in live else None for n in (k - 1, k, k + 1)]
            value = pull[k] * across_z(trio, fine_along_z)
            field[s, k] = value + keep[k] * held[s, k] if k in live else value

    own_layers, own_coarse = list(range(depth)), list(range(coarse_depth))
    all_layers, all_coarse = list(range(layers)), list(range(coarse_layers))
    nothing = jnp.zeros((coarse_rows, lanes), jnp.float32)

    def sent_on(s, guess, ks):
        for k in ks:
            if guess[k // 2] is not None:
                for side in sides:
                    field[s, k, side, :] = field[s, k, side, :] - guess[k // 2]

    @pl.when(leads)
    def _():
        rate_load.wait()
        for k in edges:
            for i in others:
                rate_copy(i, k).start()
        state_load.wait()

        @pl.when(last)
        def _():
            for i in range(parts):
                next_copy(i).start()

        prepare(own_layers)
        for k in inner:
            for i in others:
                rate_copy(i, k).start()
        spread(1, 0, own_layers)
        pl.semaphore_wait(here, 1)
        for j in range(1, groups):
            @pl.when(group - j >= 0)
            def _():
                signal(near_open if j == 1 else far_open, leader(group - j, 0))

        raw_copy().wait_recv()
        spread(0, 0, own_layers)
        drain(arrive.at[1], rates.at[pl.ds(0, len(edges) * (parts - 1))])
        near = [r * depth + k for r in others for k in edges]
        prepare(near)
        live, reach = own_layers, grown(own_layers)
        for s in (1, 0):
            settle(s, 0, live, reach)
        if inner:
            drain(arrive.at[2], rates.at[pl.ds(0, len(inner) * (parts - 1))])
        for i in others:
            hand_copy(i).start()

        @pl.when(~last)
        def _():
            pl.semaphore_wait(near_open, 1)
            for i in others:
                signal(across, leader(group, i))
            next_copy(0).start()

        prepare([k for k in all_layers if k not in own_layers + near])
        pulls, keeps = coarse_rates()
        guesses = []
        for s, gate in ((0, jnp.where(group > 0, 1.0, 0.0)), (1, None)):
            begin = [restricted(state, 2 * k, (s,)) for k in own_coarse]
            begin = begin + [None] * (coarse_layers - coarse_depth)
            guess = advance(begin, pulls, keeps, all_coarse)
            guesses.append([g if g is None or gate is None else gate * g for g in guess])
        for turn in range(1, FINE):
            live, reach = reach, grown(reach)
            for s in (0, 1):
                spread(s, turn, live)
            for s in (0, 1):
                settle(s, turn, live, reach)
        live = reach
        for s in (0, 1):
            for k in all_layers:
                if k not in live:
                    field[s, k] = jnp.zeros((rows, lanes), jnp.float32)

        def term_of(s):
            return [
                None
                if 2 * k not in live and guesses[s][k] is None
                else restricted(field, 2 * k, (s,))
                - (nothing if guesses[s][k] is None else guesses[s][k])
                for k in all_coarse
            ]

        term, after = term_of(0), term_of(1)
        run = plus(advance(term, pulls, keeps, all_coarse), after)
        run, term = ([nothing if t is None else t for t in x] for x in (run, term))
        for i in range(parts):
            shift = i * coarse_depth
            for k, c in enumerate(packed(run, shift)):
                shares[i, 0, k] = c
            for k, c in enumerate(packed(term, shift)):
                shares[i, 1, k] = c
            for k in own_coarse:
                crown[i, k] = run[(k + shift) % coarse_layers]

        @pl.when(last)
        def _():
            for i in reversed(range(parts)):
                crown_copy(i).start()

        @pl.when(~last & (group > 0))
        def _():
            for i in reversed(range(parts)):
                wrap_copy(i).start()

        for i in others:
            share_copy(i).start()

        @pl.when(~last)
        def _():
            if parts > 1:
                pl.semaphore_wait(across, parts - 1)
            for i in others:
                next_copy(i).start()

        @pl.when(group == 0)
        def _():
            for i in range(parts):
                wrap_copy(i).start()

        sent_on(1, guesses[1], all_layers)

        @pl.when(group + 2 < groups)
        def _():
            pl.semaphore_wait(far_open, groups - 2 - group)

        total, middle = packed(run), packed(term)
        drain(arrive.at[3], shares_in)
        for r in others:
            total = plus(total, [shares_in[r - 1, 0, k] for k in range(half)])
            middle = plus(middle, [shares_in[r - 1, 1, k] for k in range(half)])
        for k in range(half):
            sums[group, k] = total[k]
        for j in reversed(range(1, groups)):
            @pl.when(group + j < groups)
            def _():
                sum_copy(j).start()

        for i in others:
            part_copy(i).start()

        packed_pulls, packed_keeps = packed(pulls), packed(keeps)

        def take(index):
            drain(arrive.at[line + index], sums.at[index])

        @pl.when(group > 0)
        def _():
            take(0)

        begun = jnp.where(group > 0, 1.0, 0.0)
        coarse = tuple(begun * sums[0, k] for k in range(half))

        def pass_group(index, coarse):
            for _ in range(2):
                coarse = advance_packed(coarse, packed_pulls, packed_keeps)
            take(index)
            return tuple(plus(coarse, [sums[index, k] for k in range(half)]))

        coarse = list(lax.fori_loop(1, jnp.maximum(group, 1), pass_group, coarse))
        ahead = advance_opened(coarse, pulls, keeps)
        opened = []
        for k in own_coarse:
            both = coarse[k % half]
            opened.append(
                jnp.where(even, both, turned(both, 1, 1))
                if k < half
                else jnp.where(even, turned(both, -1, 1), both)
            )
        for k in own_coarse:
            heads[0, k] = opened[k]
            heads[1, k] = ahead[k]

        @pl.when(group > 0)
        def _():
            head_copy().start()

        finish = advance_opened(
            plus(advance_packed(coarse, packed_pulls, packed_keeps), middle), pulls, keeps
        )
        corr_copy().wait_recv()
        drain(arrive.at[4], parts_in)
        for k in own_layers:
            for side in sides:
                next_ref[0, k, side, :] = corr_in[k, side, :] + ahead[k // 2]
                held = field[1, k, side, :]
                for r in others:
                    held = held + parts_in[r - 1, k, side, :]
                end_ref[0, k, side, :] = held + finish[k // 2]
        away = pl.ds(0, depth * (parts - 1))
        drain(leave.at[0], rates.at[away])
        drain(leave.at[1], rates.at[away])
        drain(leave.at[2], state.at[1])
        drain(leave.at[4], shares_in)
        drain(leave.at[5], parts_in)
        for j in range(1, groups):
            @pl.when(groups - 1 - group == j)
            def _():
                drain(leave.at[7], sums.at[pl.ds(0, j)])

        @pl.when(last)
        def _():
            drain(leave.at[3], crown_in)

        @pl.when(~last)
        def _():
            drain(leave.at[3], wraps.at[0])

        @pl.when(group > 0)
        def _():
            drain(leave.at[6], heads)

    @pl.when(helps)
    def _():
        signal(here, leader(group, 0))
        state_load.wait()
        raw_copy().start()
        rate_load.wait()
        prepare(own_layers)
        raw_copy().wait_send()
        for i in others:
            side_copy(i).start()
        away = pl.ds(0, depth * (parts - 1))
        drain(arrive.at[2], rates.at[away])
        drain(arrive.at[1], rates.at[away])
        prepare([k for k in all_layers if k not in own_layers])
        pulls, keeps = coarse_rates()

        def solve(s, gate):
            begin = [restricted(state, 2 * k, (s,)) for k in all_coarse]
            guess = advance(begin, pulls, keeps, own_coarse)
            if gate is not None:
                guess = [g if g is None else gate * g for g in guess]
            wanted = [own_layers]
            for _ in range(1, FINE):
                wanted.append(grown(wanted[-1]))
            for turn in range(FINE):
                reach = wanted[FINE - 1 - turn]
                spread(s, turn, grown(reach))
                settle(s, turn, all_layers, reach)
            sent_on(s, guess, own_layers)

        solve(0, jnp.where(group > 0, 1.0, 0.0))
        corr_copy().start()

        def pass_group(index, coarse):
            for _ in range(2):
                coarse = advance_packed(coarse, packed_pulls, packed_keeps)
            drain(arrive.at[line + index], wraps.at[index])
            for r in range(parts):
                coarse = plus(coarse, [wraps[index, r, k] for k in range(half)])
            return tuple(coarse)

        packed_pulls, packed_keeps = packed(pulls), packed(keeps)
        midway = groups // 2

        @pl.when(group == 0)
        def _():
            coarse = lax.fori_loop(0, midway, pass_group, (nothing,) * half)
            for k in range(half):
                sums[0, k] = coarse[k]

        drain(arrive.at[0], state.at[1])
        solve(1, None)
        before = [restricted(field, 2 * k, (1,)) for k in own_coarse]
        for k in own_layers:
            for side in sides:
                next_ref[0, k, side, :] = field[1, k, side, :] - before[k // 2]
                end_ref[0, k, side, :] = field[0, k, side, :]

        @pl.when(group == 0)
        def _():
            coarse = tuple(sums[0, k] for k in range(half))
            coarse = lax.fori_loop(midway, groups - 1, pass_group, coarse)
            coarse = advance_packed(coarse, packed_pulls, packed_keeps)
            coarse = advance_opened(coarse, pulls, keeps)
            for k in own_layers:
                for side in sides:
                    next_ref[0, k, side, :] = next_ref[0, k, side, :] + coarse[k // 2]
            drain(arrive.at[line + groups - 1], crown_in)
            for k in own_layers:
                offset = crown_in[0, k // 2]
                for r in others:
                    offset = offset + crown_in[r, k // 2]
                for side in sides:
                    next_ref[0, k, side, :] = next_ref[0, k, side, :] + offset

        @pl.when(group > 0)
        def _():
            head_copy().wait_recv()
            for k in own_layers:
                for side in sides:
                    next_ref[0, k, side, :] = next_ref[0, k, side, :] + heads_in[0, k // 2]
                    end_ref[0, k, side, :] = end_ref[0, k, side, :] + heads_in[1, k // 2]

        drain(leave.at[2], corr_in)
        drain(leave.at[1], rates.at[away])


def hand_out_kernel(end_ref, next_ref, end_out, next_out, sems):
    copies = [
        pltpu.make_async_copy(end_ref, end_out, sems.at[0]),
        pltpu.make_async_copy(next_ref, next_out, sems.at[1]),
    ]
    for copy in copies:
        copy.start()
    for copy in copies:
        copy.wait()


def hand_out(end, following):
    return pl.pallas_call(
        hand_out_kernel,
        out_shape=[jax.ShapeDtypeStruct(end.shape, end.dtype)] * 2,
        in_specs=[pl.BlockSpec(memory_space=pltpu.VMEM)] * 2,
        out_specs=[pl.BlockSpec(memory_space=pl.ANY)] * 2,
        scratch_shapes=[pltpu.SemaphoreType.DMA((2,))],
    )(*(pltpu.with_memory_space_constraint(x, pltpu.VMEM) for x in (end, following)))


def solution(mesh):
    slabs, parts = mesh.shape["tm"], mesh.shape["gz"]

    def per_device(starts, cell_rates):
        depth, rows, lanes = cell_rates.shape
        layers = depth * parts
        groups = slabs // 2
        packed = (layers // 4, rows // 2, lanes)
        lead = (depth // 2, rows // 2, lanes)
        aside = max(parts - 1, 1)
        dma = pltpu.SemaphoreType.DMA

        def vmem(*shape):
            return pltpu.VMEM(shape, jnp.float32)

        ends = pl.pallas_call(
            functools.partial(kernel, slabs, parts),
            out_shape=[pltpu.VMEM(starts.shape, jnp.float32)] * 2,
            in_specs=[pl.BlockSpec(memory_space=pl.ANY)] * 2,
            out_specs=[pl.BlockSpec(memory_space=pltpu.VMEM)] * 2,
            scratch_shapes=[
                vmem(2, layers, rows, lanes),
                vmem(layers, rows, lanes),
                vmem(layers, rows, lanes),
                vmem(layers, rows, lanes),
                vmem(2, layers, rows, lanes),
                vmem(2, layers, rows, lanes),
                vmem(parts, 2, *packed),
                vmem(aside, 2, *packed),
                vmem(groups, *packed),
                vmem(groups, parts, *packed),
                vmem(parts, *lead),
                vmem(parts, *lead),
                vmem(2, *lead),
                vmem(2, *lead),
                vmem(depth, rows, lanes),
                vmem(aside, depth, rows, lanes),
                pltpu.SemaphoreType.REGULAR((4,)),
                dma((8,)),
                dma((6 + groups,)),
            ],
            compiler_params=pltpu.CompilerParams(collective_id=0, has_side_effects=True),
        )(starts, cell_rates)
        return hand_out(*ends)

    return jax.shard_map(
        per_device,
        mesh=mesh,
        in_specs=(P("tm", "gz", None, None), P("gz", None, None)),
        out_specs=(P("tm", "gz", None, None), P("tm", "gz", None, None)),
        check_vma=False,
    )
```

```python
import functools

import jax
import jax.numpy as jnp
from jax import lax
from jax.experimental import pallas as pl
from jax.experimental.pallas import tpu as pltpu
from jax.sharding import PartitionSpec as P

MESH = pl.DeviceIdType.MESH
FINE = 4
SUBLANES = 8

fine_along_z = (0.1, 0.12)
fine_along_x = (0.15, 0.12)
fine_along_y = (0.2, 0.12)
coarse_along_z = (0.2, 0.25)
coarse_along_x = (0.3, 0.25)
coarse_along_y = (0.4, 0.25)


def blend(behind, middle, beyond, along):
    courant, diffuse = along
    center = 1.0 - 2.0 * diffuse
    before, after = (diffuse + 0.5 * courant) / center, (diffuse - 0.5 * courant) / center
    if middle is None:
        return before * behind if beyond is None else after * beyond
    if behind is None:
        return middle if beyond is None else middle + after * beyond
    if beyond is None:
        return middle + before * behind
    return middle + (before * behind + after * beyond)


def centers(*alongs):
    product = 1.0
    for _, diffuse in alongs:
        product *= 1.0 - 2.0 * diffuse
    return product


def turned(values, by, dim):
    return pltpu.roll(values, by % values.shape[dim], dim)


def lane_filtered(values, by, along):
    return blend(turned(values, by, 1), values, turned(values, -by, 1), along)


def row_filtered(plane, along):
    ring = (turned(plane[-1], 1, 0), *plane, turned(plane[0], -1, 0))
    return tuple(blend(*ring[j : j + 3], along) for j in range(len(plane)))


def each(f, *planes):
    return tuple(f(*vectors) for vectors in zip(*planes))


def kernel(
    slabs, parts, starts_ref, rates_ref, end_ref, next_ref,
    state, rates, pull, keep, mixed, field, shares, shares_in, sums, wraps, crown, crown_in,
    heads, heads_in, corr_in, parts_in, base,
    ready, leave, arrive,
):
    depth, rows, lanes = rates_ref.shape
    layers = depth * parts
    groups = slabs // 2
    coarse_layers, coarse_rows, coarse_depth = layers // 2, rows // 2, depth // 2
    half = coarse_layers // 2
    vectors = rows // SUBLANES
    coarse_vectors = vectors // 2
    me, part = lax.axis_index("tm"), lax.axis_index("gz")
    group, place = me // 2, lax.rem(me, 2)
    leads, helps = place == 1, place == 0
    last = group == groups - 1

    def block(r):
        return pl.ds(r % parts * depth, depth)

    own = block(0)
    rate_load = pltpu.make_async_copy(rates_ref, rates.at[own], leave.at[5])
    state_load = pltpu.make_async_copy(starts_ref.at[0], state.at[place, own], leave.at[6])
    rate_load.start()
    state_load.start()

    def leader(g, i):
        return {"tm": 2 * g + 1, "gz": lax.rem(part + i, parts)}

    def helper(g, i):
        return {"tm": 2 * g, "gz": lax.rem(part + i, parts)}

    def signal(sem, peer):
        pl.semaphore_signal(sem, inc=1, device_id=peer, device_id_type=MESH)

    def remote(src, dst, send_sem, recv_sem, peer):
        return pltpu.make_async_remote_copy(
            src_ref=src, dst_ref=dst, send_sem=send_sem, recv_sem=recv_sem,
            device_id=peer, device_id_type=MESH,
        )

    others = range(1, parts)
    barrier = pltpu.get_barrier_semaphore()
    here, near_open, far_open, across = (ready.at[n] for n in range(4))
    line = 7

    @pl.when(leads)
    def _():
        for i in others:
            signal(barrier, leader(group, i))
        signal(barrier, helper(group, 0))
        for j in range(1, groups):
            @pl.when(group + j < groups)
            def _():
                signal(barrier, leader(group + j, 0))

    @pl.when(helps)
    def _():
        for i in others:
            signal(barrier, helper(group, i))

        @pl.when(group == 0)
        def _():
            for j in range(1, groups):
                for i in range(parts):
                    signal(barrier, leader(j, i))

    earlier = group + jnp.where(group > 0, parts, 0)
    pl.semaphore_wait(barrier, jnp.where(leads, parts - 1 + earlier, parts))

    def drain(sem, ref):
        pltpu.make_async_copy(ref, ref, sem).wait()

    def raw_copy():
        piece = state.at[0, own]
        return remote(piece, piece, leave.at[0], arrive.at[0], leader(group, 0))

    def rate_copy(i):
        return remote(
            rates.at[own], rates.at[block(parts - i)],
            leave.at[0], arrive.at[1], leader(group, i),
        )

    def hand_copy(i):
        piece = rates.at[block(i)]
        return remote(piece, piece, leave.at[1], arrive.at[1], helper(group, 0))

    def side_copy(i):
        return remote(
            state.at[0, own], state.at[0, block(parts - i)], leave.at[1], arrive.at[2], helper(group, i)
        )

    def next_copy(i):
        return remote(
            state.at[1, own], state.at[1, block(parts - i)], leave.at[2], arrive.at[0],
            helper(lax.rem(group + 1, groups), i),
        )

    def wrap_copy(i):
        return remote(
            shares.at[i, 0], wraps.at[group, (parts - i) % parts], leave.at[3], arrive.at[line + group],
            helper(0, i),
        )

    def first_copy():
        return remote(sums.at[0], wraps.at[0, 0], leave.at[3], arrive.at[line], helper(0, 0))

    def crown_copy(i):
        return remote(
            crown.at[i], crown_in.at[(parts - i) % parts], leave.at[3], arrive.at[line + group],
            helper(0, i),
        )

    def share_copy(i, n):
        return remote(
            shares.at[i, n], shares_in.at[n, parts - i - 1], leave.at[4 if n == 0 else 8],
            arrive.at[3 if n == 0 else 6], leader(group, i),
        )

    def sum_copy(j):
        piece = sums.at[group]
        return remote(piece, piece, leave.at[7], arrive.at[line + group], leader(group + j, 0))

    def part_copy(i):
        return remote(
            field.at[1, block(i)], parts_in.at[parts - i - 1], leave.at[5], arrive.at[4], leader(group, i)
        )

    def corr_copy():
        return remote(field.at[0, own], corr_in, leave.at[2], arrive.at[5], leader(group, 0))

    def head_copy():
        return remote(heads, heads_in, leave.at[6], arrive.at[3], helper(group, 0))

    even = lax.rem(lax.broadcasted_iota(jnp.int32, (SUBLANES, lanes), 1), 2) == 0
    fine_center = centers(fine_along_y, fine_along_x, fine_along_z)
    coarse_center = centers(coarse_along_y, coarse_along_x, coarse_along_z)
    strides = [pl.ds(j, SUBLANES, stride=vectors) for j in range(vectors)]

    def raw_plane(ref, *where):
        return tuple(ref[(*where, stride)] for stride in strides)

    def plane_of(ref, *where):
        return tuple(ref[(*where, j)] for j in range(ref.shape[-3]))

    def put(ref, plane, *where):
        for j, vector in enumerate(plane):
            ref[(*where, j)] = vector

    def prepare(ks):
        for k in ks:
            rate = raw_plane(rates, k)
            put(pull, each(lambda r: r * fine_center, rate), k)
            put(keep, each(lambda r: 1.0 - r, rate), k)

    def restricted(upper, lower):
        merged = each(jnp.add, upper, lower)
        averages = []
        for j in range(coarse_vectors):
            total = merged[2 * j] + merged[2 * j + 1]
            pair_sum = total + jnp.where(even, turned(total, -1, 1), turned(total, 1, 1))
            averages.append(pair_sum * 0.125)
        return tuple(averages)

    def raw_restricted(ref, k, *lead):
        return restricted(raw_plane(ref, *lead, 2 * k), raw_plane(ref, *lead, 2 * k + 1))

    def field_restricted(s, k):
        return restricted(plane_of(field, s, 2 * k), plane_of(field, s, 2 * k + 1))

    def coarse_rates(ks):
        weights = {k: raw_restricted(rates, k) for k in ks}
        return (
            {k: each(lambda v: v * coarse_center, w) for k, w in weights.items()},
            {k: each(lambda v: 1.0 - v, w) for k, w in weights.items()},
        )

    def stepped(trio, held, pulls, keeps, along):
        behind, middle, beyond = trio
        if middle is None and behind is not None and beyond is not None:
            deep = each(
                lambda b, f: blend(b, None, None, along) + blend(None, None, f, along), behind, beyond
            )
        else:
            there = [p for p in trio if p is not None]

            def mix(*given):
                given = iter(given)
                return blend(*(None if p is None else next(given) for p in trio), along)

            deep = each(mix, *there)
        if held is None:
            return each(jnp.multiply, pulls, deep)
        return each(lambda p, d, q, h: p * d + q * h, pulls, deep, keeps, held)

    def coarse_filtered(plane):
        return row_filtered(each(lambda v: lane_filtered(v, 2, coarse_along_y), plane), coarse_along_x)

    def advance(coarse, mixes, pulls, keeps, wanted):
        moved = [None] * coarse_layers
        for k in wanted:
            trio = mixes[k - 1], mixes[k], mixes[(k + 1) % coarse_layers]
            if any(p is not None for p in trio):
                moved[k] = stepped(trio, coarse[k], pulls[k], keeps[k], coarse_along_z)
        return moved

    def all_filtered(coarse):
        return [None if c is None else coarse_filtered(c) for c in coarse]

    def packed(coarse, shift=0):
        def layer(k):
            return coarse[(k + shift) % coarse_layers]

        return [each(lambda a, b: jnp.where(even, a, b), layer(k), layer(k + half)) for k in range(half)]

    def shifted(plane):
        return {n: each(lambda v: turned(v, n, 1), plane) for n in (1, 2, 3, -1, -2, -3)} | {0: plane}

    def mixed_lanes(t, even_by, odd_by):
        trio = [
            t[even_by + n]
            if even_by == odd_by
            else each(lambda a, b: jnp.where(even, a, b), t[even_by + n], t[odd_by + n])
            for n in (2, 0, -2)
        ]
        return trio[1], row_filtered(each(lambda *v: blend(*v, coarse_along_y), *trio), coarse_along_x)

    def advance_packed(coarse, pulls, keeps):
        turns = [shifted(c) for c in coarse]
        planes = [mixed_lanes(t, 0, 0)[1] for t in turns]
        low, high = mixed_lanes(turns[-1], -1, 1)[1], mixed_lanes(turns[0], -1, 1)[1]
        ring = [low] + planes + [high]
        return [
            stepped(ring[k : k + 3], coarse[k], pulls[k], keeps[k], coarse_along_z) for k in range(half)
        ]

    def advance_opened(coarse, pulls, keeps):
        turns = [shifted(c) for c in coarse]

        def opened(k):
            k = k % coarse_layers
            return mixed_lanes(turns[k % half], *((0, 1) if k < half else (-1, 0)))

        ring = [opened(k) for k in range(-1, coarse_depth + 1)]
        return [
            stepped([r[1] for r in ring[k : k + 3]], ring[k + 1][0], pulls[k], keeps[k], coarse_along_z)
            for k in range(coarse_depth)
        ]

    def open_lanes(coarse, k):
        both = coarse[k % half]
        if k < half:
            return each(lambda v: jnp.where(even, v, turned(v, 1, 1)), both)
        return each(lambda v: jnp.where(even, turned(v, -1, 1), v), both)

    def plus(first, second):
        return [
            b if a is None else a if b is None else each(jnp.add, a, b) for a, b in zip(first, second)
        ]

    def packed_in(ref, *where):
        return [plane_of(ref, *where, k) for k in range(half)]

    def grown(ks):
        return sorted({(k + n) % layers for k in ks for n in (-1, 0, 1)})

    def held_plane(s, turn, k):
        return raw_plane(state, s, k) if turn == 0 else plane_of(field, s, k)

    def spread(s, turn, ks):
        for k in ks:
            sides = each(lambda v: lane_filtered(v, 1, fine_along_y), held_plane(s, turn, k))
            put(mixed, row_filtered(sides, fine_along_x), turn % 2, s, k)

    def settle(s, turn, live, ks):
        for k in ks:
            trio = [
                plane_of(mixed, turn % 2, s, n % layers) if n % layers in live else None
                for n in (k - 1, k, k + 1)
            ]
            held = held_plane(s, turn, k) if k in live else None
            put(field, stepped(trio, held, plane_of(pull, k), plane_of(keep, k), fine_along_z), s, k)

    own_layers, own_coarse = list(range(depth)), list(range(coarse_depth))
    all_layers, all_coarse = list(range(layers)), list(range(coarse_layers))
    nothing = (jnp.zeros((SUBLANES, lanes), jnp.float32),) * coarse_vectors

    def each_fine(coarse, k):
        return tuple(coarse[k // 2][j // 2] for j in range(vectors))

    def sent_on(s, guess, ks):
        for k in ks:
            if guess[k // 2] is not None:
                put(field, each(jnp.subtract, plane_of(field, s, k), each_fine(guess, k)), s, k)

    def hand_in(ref, plane, k):
        for stride, vector in zip(strides, plane):
            ref[0, k, stride, :] = vector

    @pl.when(leads)
    def _():
        for j in range(2, groups):
            @pl.when(group - j >= 0)
            def _():
                signal(far_open, leader(group - j, 0))

        rate_load.wait()
        for i in others:
            rate_copy(i).start()
        state_load.wait()

        @pl.when(last)
        def _():
            for i in range(parts):
                next_copy(i).start()

        prepare(own_layers)
        lives = [own_layers]
        for _ in range(FINE):
            lives.append(grown(lives[-1]))
        ready_now = [own_layers]
        for turn in range(FINE):
            known = set(ready_now[-1])
            ready_now.append([
                k for k in own_layers
                if all(n % layers in known or n % layers not in lives[turn] for n in (k - 1, k, k + 1))
            ])

        def early(s):
            for turn in range(FINE):
                spread(s, turn, ready_now[turn])
                settle(s, turn, lives[turn], ready_now[turn + 1])

        def late(turn):
            for s in (0, 1):
                spread(s, turn, [k for k in lives[turn] if k not in ready_now[turn]])
            for s in (0, 1):
                settle(
                    s, turn, lives[turn], [k for k in lives[turn + 1] if k not in ready_now[turn + 1]]
                )

        def begin_of(s):
            begin = [raw_restricted(state, k, s) for k in own_coarse]
            begin += [None] * (coarse_layers - coarse_depth)
            return begin, all_filtered(begin)

        early(1)
        begins = {1: begin_of(1)}
        own_pulls, own_keeps = coarse_rates(own_coarse)
        pl.semaphore_wait(here, 1)

        @pl.when(group > 0)
        def _():
            signal(near_open, leader(group - 1, 0))

        raw_copy().wait_recv()
        early(0)
        begins[0] = begin_of(0)
        drain(arrive.at[1], rates.at[pl.ds(0, depth * (parts - 1))])
        for i in others:
            hand_copy(i).start()

        @pl.when(~last)
        def _():
            pl.semaphore_wait(near_open, 1)
            for i in others:
                signal(across, leader(group, i))
            next_copy(0).start()

        prepare([k for k in all_layers if k not in own_layers])
        for turn in range(FINE):
            late(turn)
        live = lives[-1]
        pulls, keeps = coarse_rates(all_coarse[coarse_depth:])
        pulls, keeps = own_pulls | pulls, own_keeps | keeps
        guesses = []
        for s, gate in ((0, jnp.where(group > 0, 1.0, 0.0)), (1, None)):
            guess = advance(*begins[s], pulls, keeps, all_coarse)
            if gate is not None:
                guess = [g if g is None else each(lambda v: gate * v, g) for g in guess]
            guesses.append(guess)
        for s in (0, 1):
            for k in all_layers:
                if k not in live:
                    put(field, (jnp.zeros((SUBLANES, lanes), jnp.float32),) * vectors, s, k)

        def term_of(s):
            terms = []
            for k in all_coarse:
                fine = field_restricted(s, k) if 2 * k in live else nothing
                guess = guesses[s][k]
                terms.append(fine if guess is None else each(jnp.subtract, fine, guess))
            return terms

        term, after = term_of(0), term_of(1)
        run = plus(advance(term, all_filtered(term), pulls, keeps, all_coarse), after)
        for i in range(parts):
            shift = i * coarse_depth
            for k, c in enumerate(packed(run, shift)):
                put(shares, c, i, 0, k)
            for k in own_coarse:
                put(crown, run[(k + shift) % coarse_layers], i, k)

        @pl.when(last)
        def _():
            for i in reversed(range(parts)):
                crown_copy(i).start()

        @pl.when(~last & (group > 0))
        def _():
            for i in reversed(range(parts)):
                wrap_copy(i).start()

        for i in others:
            share_copy(i, 0).start()
        for i in range(parts):
            for k, c in enumerate(packed(term, i * coarse_depth)):
                put(shares, c, i, 1, k)
        sent_on(1, guesses[1], all_layers)

        @pl.when(group + 2 < groups)
        def _():
            pl.semaphore_wait(far_open, groups - 2 - group)

        drain(arrive.at[3], shares_in.at[0])
        total = packed_in(shares, 0, 0)
        for r in others:
            total = plus(total, packed_in(shares_in, 0, r - 1))
        for k in range(half):
            put(sums, total[k], group, k)
        for j in reversed(range(1, groups)):
            @pl.when(group + j < groups)
            def _():
                sum_copy(j).start()

        @pl.when(~last)
        def _():
            if parts > 1:
                pl.semaphore_wait(across, parts - 1)
            for i in others:
                next_copy(i).start()

        @pl.when(group == 0)
        def _():
            first_copy().start()

        for i in others:
            share_copy(i, 1).start()

        packed_pulls, packed_keeps = packed(pulls), packed(keeps)

        def twice(coarse):
            for _ in range(2):
                coarse = advance_packed(coarse, packed_pulls, packed_keeps)
            return coarse

        @pl.when(group > 0)
        def _():
            drain(arrive.at[line], sums.at[0])

        for i in others:
            part_copy(i).start()

        @pl.when(group == 0)
        def _():
            for k in range(half):
                put(base, nothing, k)

        @pl.when(group > 0)
        def _():
            def pass_group(index, coarse):
                coarse = twice(coarse)
                drain(arrive.at[line + index], sums.at[index])
                return plus(coarse, packed_in(sums, index))

            coarse = lax.fori_loop(1, group, pass_group, packed_in(sums, 0))
            for k in range(half):
                put(base, coarse[k], k)

        coarse = packed_in(base)
        ahead = advance_opened(coarse, pulls, keeps)

        @pl.when(group > 0)
        def _():
            for k in own_coarse:
                put(heads, open_lanes(coarse, k), 0, k)
                put(heads, ahead[k], 1, k)
            head_copy().start()

        drain(arrive.at[6], shares_in.at[1])
        middle = packed_in(shares, 0, 1)
        for r in others:
            middle = plus(middle, packed_in(shares_in, 1, r - 1))
        finish = advance_opened(
            plus(advance_packed(coarse, packed_pulls, packed_keeps), middle), pulls, keeps
        )
        corr_copy().wait_recv()
        drain(arrive.at[4], parts_in)
        for k in own_layers:
            hand_in(next_ref, each(jnp.add, plane_of(corr_in, k), each_fine(ahead, k)), k)
            held = plane_of(field, 1, k)
            for r in others:
                held = each(jnp.add, held, plane_of(parts_in, r - 1, k))
            hand_in(end_ref, each(jnp.add, held, each_fine(finish, k)), k)
        away = pl.ds(0, depth * (parts - 1))
        drain(leave.at[0], rates.at[away])
        drain(leave.at[1], rates.at[away])
        drain(leave.at[2], state.at[1])
        drain(leave.at[4], shares_in.at[0])
        drain(leave.at[8], shares_in.at[1])
        drain(leave.at[5], parts_in)
        for j in range(1, groups):
            @pl.when(groups - 1 - group == j)
            def _():
                drain(leave.at[7], sums.at[pl.ds(0, j)])

        @pl.when(last)
        def _():
            drain(leave.at[3], crown_in)

        @pl.when(~last & (group > 0))
        def _():
            drain(leave.at[3], wraps.at[0])

        @pl.when(group == 0)
        def _():
            drain(leave.at[3], sums.at[0])

        @pl.when(group > 0)
        def _():
            drain(leave.at[6], heads)

    @pl.when(helps)
    def _():
        signal(here, leader(group, 0))
        state_load.wait()
        raw_copy().start()
        rate_load.wait()
        prepare(own_layers)
        raw_copy().wait_send()
        for i in others:
            side_copy(i).start()
        away = pl.ds(0, depth * (parts - 1))
        drain(arrive.at[2], rates.at[away])
        drain(arrive.at[1], rates.at[away])
        prepare([k for k in all_layers if k not in own_layers])
        pulls, keeps = coarse_rates(all_coarse)

        def solve(s, gate):
            begin = [raw_restricted(state, k, s) for k in all_coarse]
            guess = advance(begin, all_filtered(begin), pulls, keeps, own_coarse)
            if gate is not None:
                guess = [g if g is None else each(lambda v: gate * v, g) for g in guess]
            wanted = [own_layers]
            for _ in range(1, FINE):
                wanted.append(grown(wanted[-1]))
            for turn in range(FINE):
                reach = wanted[FINE - 1 - turn]
                spread(s, turn, grown(reach))
                settle(s, turn, all_layers, reach)
            sent_on(s, guess, own_layers)

        solve(0, jnp.where(group > 0, 1.0, 0.0))
        corr_copy().start()
        packed_pulls, packed_keeps = packed(pulls), packed(keeps)

        def arrived(index):
            drain(arrive.at[line + index], wraps.at[index])

        def with_arrived(coarse, index):
            for r in range(parts):
                coarse = plus(coarse, packed_in(wraps, index, r))
            return coarse

        def twice(coarse):
            for _ in range(2):
                coarse = advance_packed(coarse, packed_pulls, packed_keeps)
            return coarse

        def second_solve():
            solve(1, None)
            before = [field_restricted(1, k) for k in own_coarse]
            sent_on(1, before, own_layers)

        @pl.when(group == 0)
        def _():
            for k in own_layers:
                hand_in(end_ref, plane_of(field, 0, k), k)
            drain(arrive.at[line], wraps.at[0, 0])
            coarse = twice(packed_in(wraps, 0, 0))
            midway = max(groups - 3, 1)
            for index in range(1, midway):
                arrived(index)
            drain(arrive.at[0], state.at[1])
            for index in range(1, midway):
                coarse = twice(with_arrived(coarse, index))
            second_solve()
            for index in range(midway, groups - 1):
                arrived(index)
                coarse = with_arrived(coarse, index)
                if index < groups - 2:
                    coarse = twice(coarse)
            coarse = advance_packed(coarse, packed_pulls, packed_keeps)
            coarse = advance_opened(coarse, pulls, keeps)
            for k in own_layers:
                put(field, each(jnp.add, plane_of(field, 1, k), each_fine(coarse, k)), 1, k)
            drain(arrive.at[line + groups - 1], crown_in)
            for k in own_layers:
                following = plane_of(field, 1, k)
                for r in range(parts):
                    offset = each_fine([plane_of(crown_in, r, c) for c in own_coarse], k)
                    following = each(jnp.add, following, offset)
                hand_in(next_ref, following, k)

        @pl.when(group > 0)
        def _():
            drain(arrive.at[0], state.at[1])
            second_solve()
            head_copy().wait_recv()
            for k in own_layers:
                coarse, ahead = ([plane_of(heads_in, n, c) for c in own_coarse] for n in range(2))
                hand_in(next_ref, each(jnp.add, plane_of(field, 1, k), each_fine(coarse, k)), k)
                hand_in(end_ref, each(jnp.add, plane_of(field, 0, k), each_fine(ahead, k)), k)

        drain(leave.at[2], corr_in)
        drain(leave.at[1], rates.at[away])


def hand_out_kernel(end_ref, next_ref, end_out, next_out, sems):
    copies = [
        pltpu.make_async_copy(end_ref, end_out, sems.at[0]),
        pltpu.make_async_copy(next_ref, next_out, sems.at[1]),
    ]
    for copy in copies:
        copy.start()
    for copy in copies:
        copy.wait()


def hand_out(end, following):
    return pl.pallas_call(
        hand_out_kernel,
        out_shape=[jax.ShapeDtypeStruct(end.shape, end.dtype)] * 2,
        in_specs=[pl.BlockSpec(memory_space=pltpu.VMEM)] * 2,
        out_specs=[pl.BlockSpec(memory_space=pl.ANY)] * 2,
        scratch_shapes=[pltpu.SemaphoreType.DMA((2,))],
    )(*(pltpu.with_memory_space_constraint(x, pltpu.VMEM) for x in (end, following)))


def solution(mesh):
    slabs, parts = mesh.shape["tm"], mesh.shape["gz"]

    def per_device(starts, cell_rates):
        depth, rows, lanes = cell_rates.shape
        layers = depth * parts
        groups = slabs // 2
        vectors = rows // SUBLANES
        fine = (vectors, SUBLANES, lanes)
        coarse = (vectors // 2, SUBLANES, lanes)
        packed = (layers // 4, *coarse)
        lead = (depth // 2, *coarse)
        aside = max(parts - 1, 1)
        dma = pltpu.SemaphoreType.DMA

        def vmem(*shape):
            return pltpu.VMEM(shape, jnp.float32)

        ends = pl.pallas_call(
            functools.partial(kernel, slabs, parts),
            out_shape=[pltpu.VMEM(starts.shape, jnp.float32)] * 2,
            in_specs=[pl.BlockSpec(memory_space=pl.ANY)] * 2,
            out_specs=[pl.BlockSpec(memory_space=pltpu.VMEM)] * 2,
            scratch_shapes=[
                vmem(2, layers, rows, lanes),
                vmem(layers, rows, lanes),
                vmem(layers, *fine),
                vmem(layers, *fine),
                vmem(2, 2, layers, *fine),
                vmem(2, layers, *fine),
                vmem(parts, 2, *packed),
                vmem(2, aside, *packed),
                vmem(groups, *packed),
                vmem(groups, parts, *packed),
                vmem(parts, *lead),
                vmem(parts, *lead),
                vmem(2, *lead),
                vmem(2, *lead),
                vmem(depth, *fine),
                vmem(aside, depth, *fine),
                vmem(*packed),
                pltpu.SemaphoreType.REGULAR((4,)),
                dma((9,)),
                dma((7 + groups,)),
            ],
            compiler_params=pltpu.CompilerParams(collective_id=0, has_side_effects=True),
        )(starts, cell_rates)
        return hand_out(*ends)

    return jax.shard_map(
        per_device,
        mesh=mesh,
        in_specs=(P("tm", "gz", None, None), P("gz", None, None)),
        out_specs=(P("tm", "gz", None, None), P("tm", "gz", None, None)),
        check_vma=False,
    )
```

```python
import functools

import jax
import jax.numpy as jnp
from jax import lax
from jax.experimental import pallas as pl
from jax.experimental.pallas import tpu as pltpu
from jax.sharding import PartitionSpec as P

MESH = pl.DeviceIdType.MESH
FINE = 4
SUBLANES = 8

fine_along_z = (0.1, 0.12)
fine_along_x = (0.15, 0.12)
fine_along_y = (0.2, 0.12)
coarse_along_z = (0.2, 0.25)
coarse_along_x = (0.3, 0.25)
coarse_along_y = (0.4, 0.25)


def blend(behind, middle, beyond, along):
    courant, diffuse = along
    center = 1.0 - 2.0 * diffuse
    before, after = (diffuse + 0.5 * courant) / center, (diffuse - 0.5 * courant) / center
    if middle is None:
        return before * behind if beyond is None else after * beyond
    if behind is None:
        return middle if beyond is None else middle + after * beyond
    if beyond is None:
        return middle + before * behind
    return middle + (before * behind + after * beyond)


def centers(*alongs):
    product = 1.0
    for _, diffuse in alongs:
        product *= 1.0 - 2.0 * diffuse
    return product


def turned(values, by, dim):
    return pltpu.roll(values, by % values.shape[dim], dim)


def lane_filtered(values, by, along):
    return blend(turned(values, by, 1), values, turned(values, -by, 1), along)


def row_filtered(plane, along):
    ring = (turned(plane[-1], 1, 0), *plane, turned(plane[0], -1, 0))
    return tuple(blend(*ring[j : j + 3], along) for j in range(len(plane)))


def each(f, *planes):
    return tuple(f(*vectors) for vectors in zip(*planes))


def kernel(
    slabs, parts, starts_ref, rates_ref, end_ref, next_ref,
    state, rates, pull, keep, mixed, field, shares, shares_in, sums, wraps, crown, crown_in,
    heads, heads_in, corr_in, parts_in, base, raw_in,
    ready, leave, arrive,
):
    depth, rows, lanes = rates_ref.shape
    layers = depth * parts
    groups = slabs // 2
    coarse_layers, coarse_rows, coarse_depth = layers // 2, rows // 2, depth // 2
    half = coarse_layers // 2
    vectors = rows // SUBLANES
    coarse_vectors = vectors // 2
    me, part = lax.axis_index("tm"), lax.axis_index("gz")
    group, place = me // 2, lax.rem(me, 2)
    leads, helps = place == 1, place == 0
    last = group == groups - 1
    direct, proxy = (group == 0) & (part == 0), (group == 0) & (part > 0)

    def block(r):
        return pl.ds(r % parts * depth, depth)

    own = block(0)
    rate_load = pltpu.make_async_copy(rates_ref, rates.at[own], leave.at[5])
    state_load = pltpu.make_async_copy(starts_ref.at[0], state.at[place, own], leave.at[6])
    rate_load.start()
    state_load.start()

    def leader(g, i):
        return {"tm": 2 * g + 1, "gz": lax.rem(part + i, parts)}

    def helper(g, i):
        return {"tm": 2 * g, "gz": lax.rem(part + i, parts)}

    def signal(sem, peer):
        pl.semaphore_signal(sem, inc=1, device_id=peer, device_id_type=MESH)

    def remote(src, dst, send_sem, recv_sem, peer):
        return pltpu.make_async_remote_copy(
            src_ref=src, dst_ref=dst, send_sem=send_sem, recv_sem=recv_sem,
            device_id=peer, device_id_type=MESH,
        )

    others = range(1, parts)
    barrier = pltpu.get_barrier_semaphore()
    here, near_open, far_open, across = (ready.at[n] for n in range(4))
    line = 8

    @pl.when(leads)
    def _():
        for i in others:
            signal(barrier, leader(group, i))
        signal(barrier, helper(group, 0))
        for j in range(1, groups):
            @pl.when(group + j < groups)
            def _():
                signal(barrier, leader(group + j, 0))

        @pl.when(proxy)
        def _():
            for j in range(1, groups):
                for i in others:
                    signal(barrier, leader(j, i))

    @pl.when(helps)
    def _():
        for i in others:
            signal(barrier, helper(group, i))

        @pl.when(direct)
        def _():
            for j in range(1, groups):
                for i in range(parts):
                    signal(barrier, leader(j, i))

    earlier = group + jnp.where(group > 0, parts - jnp.where(part > 0, 1, 0), 0)
    pl.semaphore_wait(barrier, jnp.where(leads, parts - 1 + earlier, parts))

    def drain(sem, ref):
        pltpu.make_async_copy(ref, ref, sem).wait()

    def raw_copy():
        piece = state.at[0, own]
        return remote(piece, piece, leave.at[0], arrive.at[0], leader(group, 0))

    def rate_copy(i):
        return remote(
            rates.at[own], rates.at[block(parts - i)],
            leave.at[0], arrive.at[1], leader(group, i),
        )

    def hand_copy(i):
        piece = rates.at[block(i)]
        return remote(piece, piece, leave.at[1], arrive.at[1], helper(group, 0))

    def side_copy(i):
        return remote(
            state.at[0, own], state.at[0, block(parts - i)], leave.at[1], arrive.at[2], helper(group, i)
        )

    def offset_to(q):
        return lax.rem(q + parts - part, parts)

    def home(i):
        q = lax.rem(part + i, parts)
        return {"tm": jnp.where(q == 0, 0, 1), "gz": q}

    def raw_next(i, send_sem, peer):
        r = lax.rem(parts - i, parts)
        return remote(state.at[1, own], raw_in.at[pl.ds(r * depth, depth)], send_sem, arrive.at[7], peer)

    def next_copy(i):
        return raw_next(i, leave.at[2], helper(group + 1, i))

    def round_copy(i):
        return raw_next(i, leave.at[2], home(i))

    def forward_copy():
        return remote(raw_in, raw_in, leave.at[3], arrive.at[7], helper(0, 0))

    def wrap_copy(i):
        return remote(
            shares.at[i, 0], wraps.at[group, lax.rem(parts - i, parts)], leave.at[3], arrive.at[line + group],
            home(i),
        )

    def first_copy():
        return remote(sums.at[0], wraps.at[0, 0], leave.at[3], arrive.at[line], helper(0, 0))

    def crown_copy(i):
        return remote(
            crown.at[i], crown_in.at[lax.rem(parts - i, parts)], leave.at[3], arrive.at[line + group],
            home(i),
        )

    def share_copy(i, n):
        return remote(
            shares.at[i, n], shares_in.at[n, parts - i - 1], leave.at[4 if n == 0 else 8],
            arrive.at[3 if n == 0 else 6], leader(group, i),
        )

    def sum_copy(j):
        piece = sums.at[group]
        return remote(piece, piece, leave.at[7], arrive.at[line + group], leader(group + j, 0))

    def part_copy(i):
        return remote(
            field.at[1, block(i)], parts_in.at[parts - i - 1], leave.at[5], arrive.at[4], leader(group, i)
        )

    def corr_copy():
        return remote(field.at[0, own], corr_in, leave.at[2], arrive.at[5], leader(group, 0))

    def head_copy():
        return remote(heads, heads_in, leave.at[6], arrive.at[3], helper(group, 0))

    even = lax.rem(lax.broadcasted_iota(jnp.int32, (SUBLANES, lanes), 1), 2) == 0
    fine_center = centers(fine_along_y, fine_along_x, fine_along_z)
    coarse_center = centers(coarse_along_y, coarse_along_x, coarse_along_z)
    strides = [pl.ds(j, SUBLANES, stride=vectors) for j in range(vectors)]

    def raw_plane(ref, *where):
        return tuple(ref[(*where, stride)] for stride in strides)

    def plane_of(ref, *where):
        return tuple(ref[(*where, j)] for j in range(ref.shape[-3]))

    def put(ref, plane, *where):
        for j, vector in enumerate(plane):
            ref[(*where, j)] = vector

    def prepare(ks):
        for k in ks:
            rate = raw_plane(rates, k)
            put(pull, each(lambda r: r * fine_center, rate), k)
            put(keep, each(lambda r: 1.0 - r, rate), k)

    def restricted(upper, lower):
        merged = each(jnp.add, upper, lower)
        averages = []
        for j in range(coarse_vectors):
            total = merged[2 * j] + merged[2 * j + 1]
            pair_sum = total + jnp.where(even, turned(total, -1, 1), turned(total, 1, 1))
            averages.append(pair_sum * 0.125)
        return tuple(averages)

    def restricted_and_filtered(upper, lower, guess):
        merged = each(jnp.add, upper, lower)
        total = tuple(merged[2 * j] + merged[2 * j + 1] for j in range(coarse_vectors))
        if guess is not None:
            total = each(lambda t, g: t - 4.0 * g, total, guess)
        total = each(lambda t: t * 0.125, total)
        t = shifted(total)

        def pair(n):
            return each(lambda here, a, b: here + jnp.where(even, a, b), t[n], t[n - 1], t[n + 1])

        here = pair(0)
        sides = each(lambda *v: blend(*v, coarse_along_y), pair(2), here, pair(-2))
        return here, row_filtered(sides, coarse_along_x)

    def raw_restricted(ref, k, *lead):
        return restricted(raw_plane(ref, *lead, 2 * k), raw_plane(ref, *lead, 2 * k + 1))

    def field_restricted(s, k):
        return restricted(plane_of(field, s, 2 * k), plane_of(field, s, 2 * k + 1))

    def coarse_rates(ks):
        weights = {k: raw_restricted(rates, k) for k in ks}
        return (
            {k: each(lambda v: v * coarse_center, w) for k, w in weights.items()},
            {k: each(lambda v: 1.0 - v, w) for k, w in weights.items()},
        )

    def stepped(trio, held, pulls, keeps, along):
        behind, middle, beyond = trio
        if middle is None and behind is not None and beyond is not None:
            deep = each(
                lambda b, f: blend(b, None, None, along) + blend(None, None, f, along), behind, beyond
            )
        else:
            there = [p for p in trio if p is not None]

            def mix(*given):
                given = iter(given)
                return blend(*(None if p is None else next(given) for p in trio), along)

            deep = each(mix, *there)
        if held is None:
            return each(jnp.multiply, pulls, deep)
        return each(lambda p, d, q, h: p * d + q * h, pulls, deep, keeps, held)

    def coarse_filtered(plane):
        return row_filtered(each(lambda v: lane_filtered(v, 2, coarse_along_y), plane), coarse_along_x)

    def advance(coarse, mixes, pulls, keeps, wanted):
        moved = [None] * coarse_layers
        for k in wanted:
            trio = mixes[k - 1], mixes[k], mixes[(k + 1) % coarse_layers]
            if any(p is not None for p in trio):
                moved[k] = stepped(trio, coarse[k], pulls[k], keeps[k], coarse_along_z)
        return moved

    def all_filtered(coarse):
        return [None if c is None else coarse_filtered(c) for c in coarse]

    def packed(coarse, shift=0):
        def layer(k):
            return coarse[(k + shift) % coarse_layers]

        return [each(lambda a, b: jnp.where(even, a, b), layer(k), layer(k + half)) for k in range(half)]

    def shifted(plane):
        return {n: each(lambda v: turned(v, n, 1), plane) for n in (1, 2, 3, -1, -2, -3)} | {0: plane}

    def mixed_lanes(t, even_by, odd_by):
        trio = [
            t[even_by + n]
            if even_by == odd_by
            else each(lambda a, b: jnp.where(even, a, b), t[even_by + n], t[odd_by + n])
            for n in (2, 0, -2)
        ]
        return trio[1], row_filtered(each(lambda *v: blend(*v, coarse_along_y), *trio), coarse_along_x)

    def advance_packed(coarse, pulls, keeps):
        turns = [shifted(c) for c in coarse]
        planes = [mixed_lanes(t, 0, 0)[1] for t in turns]
        low, high = mixed_lanes(turns[-1], -1, 1)[1], mixed_lanes(turns[0], -1, 1)[1]
        ring = [low] + planes + [high]
        return [
            stepped(ring[k : k + 3], coarse[k], pulls[k], keeps[k], coarse_along_z) for k in range(half)
        ]

    def advance_opened(coarse, pulls, keeps):
        turns = [shifted(c) for c in coarse]

        def opened(k):
            k = k % coarse_layers
            return mixed_lanes(turns[k % half], *((0, 1) if k < half else (-1, 0)))

        ring = [opened(k) for k in range(-1, coarse_depth + 1)]
        return [
            stepped([r[1] for r in ring[k : k + 3]], ring[k + 1][0], pulls[k], keeps[k], coarse_along_z)
            for k in range(coarse_depth)
        ]

    def open_lanes(coarse, k):
        both = coarse[k % half]
        if k < half:
            return each(lambda v: jnp.where(even, v, turned(v, 1, 1)), both)
        return each(lambda v: jnp.where(even, turned(v, -1, 1), v), both)

    def plus(first, second):
        return [
            b if a is None else a if b is None else each(jnp.add, a, b) for a, b in zip(first, second)
        ]

    def packed_in(ref, *where):
        return [plane_of(ref, *where, k) for k in range(half)]

    def grown(ks):
        return sorted({(k + n) % layers for k in ks for n in (-1, 0, 1)})

    def origin(s, k):
        return raw_plane(state, s, k)

    def held_plane(s, turn, k, first):
        return first(s, k) if turn == 0 else plane_of(field, s, k)

    def spread(s, turn, ks, first=origin):
        for k in ks:
            sides = each(lambda v: lane_filtered(v, 1, fine_along_y), held_plane(s, turn, k, first))
            put(mixed, row_filtered(sides, fine_along_x), turn % 2, s, k)

    def settle(s, turn, live, ks, first=origin):
        for k in ks:
            trio = [
                plane_of(mixed, turn % 2, s, n % layers) if n % layers in live else None
                for n in (k - 1, k, k + 1)
            ]
            held = held_plane(s, turn, k, first) if k in live else None
            put(field, stepped(trio, held, plane_of(pull, k), plane_of(keep, k), fine_along_z), s, k)

    own_layers, own_coarse = list(range(depth)), list(range(coarse_depth))
    all_layers, all_coarse = list(range(layers)), list(range(coarse_layers))
    nothing = (jnp.zeros((SUBLANES, lanes), jnp.float32),) * coarse_vectors

    def each_fine(coarse, k):
        return tuple(coarse[k // 2][j // 2] for j in range(vectors))

    def sent_on(s, guess, ks):
        for k in ks:
            if guess[k // 2] is not None:
                put(field, each(jnp.subtract, plane_of(field, s, k), each_fine(guess, k)), s, k)

    def hand_in(ref, plane, k):
        for stride, vector in zip(strides, plane):
            ref[0, k, stride, :] = vector

    @pl.when(leads)
    def _():
        for j in range(2, groups):
            @pl.when(group - j >= 0)
            def _():
                signal(far_open, leader(group - j, 0))

        rate_load.wait()
        for i in others:
            rate_copy(i).start()
        state_load.wait()

        @pl.when(last)
        def _():
            for q in range(parts):
                round_copy(offset_to(q)).start()

        prepare(own_layers)
        lives = [own_layers]
        for _ in range(FINE):
            lives.append(grown(lives[-1]))
        ready_now = [own_layers]
        for turn in range(FINE):
            known = set(ready_now[-1])
            ready_now.append([
                k for k in own_layers
                if all(n % layers in known or n % layers not in lives[turn] for n in (k - 1, k, k + 1))
            ])

        def early(s):
            for turn in range(FINE):
                spread(s, turn, ready_now[turn])
                settle(s, turn, lives[turn], ready_now[turn + 1])

        def late(turn):
            for s in (0, 1):
                spread(s, turn, [k for k in lives[turn] if k not in ready_now[turn]])
            for s in (0, 1):
                settle(
                    s, turn, lives[turn], [k for k in lives[turn + 1] if k not in ready_now[turn + 1]]
                )

        def begin_of(s):
            begin = [raw_restricted(state, k, s) for k in own_coarse]
            begin += [None] * (coarse_layers - coarse_depth)
            return begin, all_filtered(begin)

        early(1)
        begins = {1: begin_of(1)}
        own_pulls, own_keeps = coarse_rates(own_coarse)
        pl.semaphore_wait(here, 1)

        @pl.when(group > 0)
        def _():
            signal(near_open, leader(group - 1, 0))

        raw_copy().wait_recv()
        early(0)
        begins[0] = begin_of(0)
        drain(arrive.at[1], rates.at[pl.ds(0, depth * (parts - 1))])
        for i in others:
            hand_copy(i).start()

        @pl.when(~last)
        def _():
            pl.semaphore_wait(near_open, 1)
            for i in others:
                signal(across, leader(group, i))
            next_copy(0).start()

        prepare([k for k in all_layers if k not in own_layers])
        for turn in range(FINE):
            late(turn)
        live = lives[-1]
        pulls, keeps = coarse_rates(all_coarse[coarse_depth:])
        pulls, keeps = own_pulls | pulls, own_keeps | keeps
        guesses = []
        for s, gate in ((0, jnp.where(group > 0, 1.0, 0.0)), (1, None)):
            guess = advance(*begins[s], pulls, keeps, all_coarse)
            if gate is not None:
                guess = [g if g is None else each(lambda v: gate * v, g) for g in guess]
            guesses.append(guess)
        for s in (0, 1):
            for k in all_layers:
                if k not in live:
                    put(field, (jnp.zeros((SUBLANES, lanes), jnp.float32),) * vectors, s, k)

        def fine_of(s, k):
            return plane_of(field, s, 2 * k), plane_of(field, s, 2 * k + 1)

        def zero_guess(s, k):
            return guesses[s][k] if guesses[s][k] is not None else nothing

        both = [
            restricted_and_filtered(*fine_of(0, k), guesses[0][k])
            if 2 * k in live
            else (each(jnp.negative, zero_guess(0, k)), coarse_filtered(each(jnp.negative, zero_guess(0, k))))
            for k in all_coarse
        ]
        term = [b[0] for b in both]
        after = [
            each(jnp.subtract, restricted(*fine_of(1, k)) if 2 * k in live else nothing, zero_guess(1, k))
            for k in all_coarse
        ]
        run = plus(advance(term, [b[1] for b in both], pulls, keeps, all_coarse), after)
        for i in range(parts):
            shift = i * coarse_depth
            for k, c in enumerate(packed(run, shift)):
                put(shares, c, i, 0, k)
            for k in own_coarse:
                put(crown, run[(k + shift) % coarse_layers], i, k)

        @pl.when(last)
        def _():
            for q in range(parts):
                crown_copy(offset_to(q)).start()

        @pl.when(~last & (group > 0))
        def _():
            for q in range(parts):
                wrap_copy(offset_to(q)).start()

        for i in others:
            share_copy(i, 0).start()
        for i in range(parts):
            for k, c in enumerate(packed(term, i * coarse_depth)):
                put(shares, c, i, 1, k)
        sent_on(1, guesses[1], all_layers)

        @pl.when(group == 0)
        def _():
            for i in others:
                part_copy(i).start()
                share_copy(i, 1).start()

        @pl.when(group + 2 < groups)
        def _():
            pl.semaphore_wait(far_open, groups - 2 - group)

        drain(arrive.at[3], shares_in.at[0])
        total = packed_in(shares, 0, 0)
        for r in others:
            total = plus(total, packed_in(shares_in, 0, r - 1))
        for k in range(half):
            put(sums, total[k], group, k)
        for j in reversed(range(1, groups)):
            @pl.when(group + j < groups)
            def _():
                sum_copy(j).start()

        @pl.when(~last)
        def _():
            if parts > 1:
                pl.semaphore_wait(across, parts - 1)
            for i in others:
                next_copy(i).start()

        @pl.when(direct)
        def _():
            first_copy().start()

        @pl.when(group > 0)
        def _():
            for i in others:
                share_copy(i, 1).start()

        packed_pulls, packed_keeps = packed(pulls), packed(keeps)

        def twice(coarse):
            for _ in range(2):
                coarse = advance_packed(coarse, packed_pulls, packed_keeps)
            return coarse

        @pl.when(group > 0)
        def _():
            drain(arrive.at[line], sums.at[0])
            for i in others:
                part_copy(i).start()

        @pl.when(group == 0)
        def _():
            for k in range(half):
                put(base, nothing, k)

        @pl.when(group > 0)
        def _():
            def pass_group(index, coarse):
                coarse = twice(coarse)
                drain(arrive.at[line + index], sums.at[index])
                return plus(coarse, packed_in(sums, index))

            coarse = lax.fori_loop(1, group, pass_group, packed_in(sums, 0))
            for k in range(half):
                put(base, coarse[k], k)

        coarse = packed_in(base)
        ahead = advance_opened(coarse, pulls, keeps)

        @pl.when(group > 0)
        def _():
            for k in own_coarse:
                put(heads, open_lanes(coarse, k), 0, k)
                put(heads, ahead[k], 1, k)
            head_copy().start()

        drain(arrive.at[6], shares_in.at[1])
        middle = packed_in(shares, 0, 1)
        for r in others:
            middle = plus(middle, packed_in(shares_in, 1, r - 1))
        finish = advance_opened(
            plus(advance_packed(coarse, packed_pulls, packed_keeps), middle), pulls, keeps
        )
        corr_copy().wait_recv()
        drain(arrive.at[4], parts_in)
        for k in own_layers:
            hand_in(next_ref, each(jnp.add, plane_of(corr_in, k), each_fine(ahead, k)), k)
            held = plane_of(field, 1, k)
            for r in others:
                held = each(jnp.add, held, plane_of(parts_in, r - 1, k))
            hand_in(end_ref, each(jnp.add, held, each_fine(finish, k)), k)
        away = pl.ds(0, depth * (parts - 1))
        drain(leave.at[0], rates.at[away])
        drain(leave.at[1], rates.at[away])
        drain(leave.at[2], raw_in)
        drain(leave.at[4], shares_in.at[0])
        drain(leave.at[8], shares_in.at[1])
        drain(leave.at[5], parts_in)
        for j in range(1, groups):
            @pl.when(groups - 1 - group == j)
            def _():
                drain(leave.at[7], sums.at[pl.ds(0, j)])

        @pl.when(last)
        def _():
            drain(leave.at[3], crown_in)

        @pl.when(~last & (group > 0))
        def _():
            drain(leave.at[3], wraps.at[0])

        @pl.when(direct)
        def _():
            drain(leave.at[3], sums.at[0])

        @pl.when(proxy)
        def _():
            drain(arrive.at[7], raw_in)
            forward_copy().start()

            def pass_group(index, coarse):
                coarse = twice(coarse)
                drain(arrive.at[line + index], wraps.at[index])
                for r in range(parts):
                    coarse = plus(coarse, packed_in(wraps, index, r))
                return coarse

            coarse = lax.fori_loop(1, groups - 1, pass_group, packed_in(sums, 0))
            coarse = advance_packed(coarse, packed_pulls, packed_keeps)
            coarse = advance_opened(coarse, pulls, keeps)
            drain(arrive.at[line + groups - 1], crown_in)
            for k in own_coarse:
                following = coarse[k]
                for r in range(parts):
                    following = each(jnp.add, following, plane_of(crown_in, r, k))
                put(heads, following, 0, k)
                put(heads, nothing, 1, k)
            head_copy().start()
            drain(leave.at[3], raw_in)

        @pl.when(~direct)
        def _():
            drain(leave.at[6], heads)

    @pl.when(helps)
    def _():
        signal(here, leader(group, 0))
        state_load.wait()
        raw_copy().start()
        rate_load.wait()
        prepare(own_layers)
        raw_copy().wait_send()
        for i in others:
            side_copy(i).start()
        away = pl.ds(0, depth * (parts - 1))
        drain(arrive.at[2], rates.at[away])
        drain(arrive.at[1], rates.at[away])
        prepare([k for k in all_layers if k not in own_layers])
        pulls, keeps = coarse_rates(all_coarse)

        def solve(s, gate):
            def first(s, k):
                return raw_plane(state, 0, k) if s == 0 else raw_plane(raw_in, k)

            begin = [restricted(first(s, 2 * k), first(s, 2 * k + 1)) for k in all_coarse]
            guess = advance(begin, all_filtered(begin), pulls, keeps, own_coarse)
            if gate is not None:
                guess = [g if g is None else each(lambda v: gate * v, g) for g in guess]
            wanted = [own_layers]
            for _ in range(1, FINE):
                wanted.append(grown(wanted[-1]))
            for turn in range(FINE):
                reach = wanted[FINE - 1 - turn]
                spread(s, turn, grown(reach), first)
                settle(s, turn, all_layers, reach, first)
            sent_on(s, guess, own_layers)

        solve(0, jnp.where(group > 0, 1.0, 0.0))
        corr_copy().start()
        packed_pulls, packed_keeps = packed(pulls), packed(keeps)

        def arrived(index):
            drain(arrive.at[line + index], wraps.at[index])

        def with_arrived(coarse, index):
            for r in range(parts):
                coarse = plus(coarse, packed_in(wraps, index, r))
            return coarse

        def twice(coarse):
            for _ in range(2):
                coarse = advance_packed(coarse, packed_pulls, packed_keeps)
            return coarse

        def second_solve():
            solve(1, None)
            before = [field_restricted(1, k) for k in own_coarse]
            sent_on(1, before, own_layers)

        @pl.when(direct)
        def _():
            for k in own_layers:
                hand_in(end_ref, plane_of(field, 0, k), k)
            drain(arrive.at[line], wraps.at[0, 0])
            coarse = twice(packed_in(wraps, 0, 0))
            midway = max(groups - 3, 1)
            for index in range(1, midway):
                arrived(index)
            drain(arrive.at[7], raw_in)
            for index in range(1, midway):
                coarse = twice(with_arrived(coarse, index))
            second_solve()
            for index in range(midway, groups - 1):
                arrived(index)
                coarse = with_arrived(coarse, index)
                if index < groups - 2:
                    coarse = twice(coarse)
            coarse = advance_packed(coarse, packed_pulls, packed_keeps)
            coarse = advance_opened(coarse, pulls, keeps)
            for k in own_layers:
                put(field, each(jnp.add, plane_of(field, 1, k), each_fine(coarse, k)), 1, k)
            drain(arrive.at[line + groups - 1], crown_in)
            for k in own_layers:
                following = plane_of(field, 1, k)
                for r in range(parts):
                    offset = each_fine([plane_of(crown_in, r, c) for c in own_coarse], k)
                    following = each(jnp.add, following, offset)
                hand_in(next_ref, following, k)

        @pl.when(~direct)
        def _():
            drain(arrive.at[7], raw_in)
            second_solve()
            head_copy().wait_recv()
            for k in own_layers:
                coarse, ahead = ([plane_of(heads_in, n, c) for c in own_coarse] for n in range(2))
                hand_in(next_ref, each(jnp.add, plane_of(field, 1, k), each_fine(coarse, k)), k)
                hand_in(end_ref, each(jnp.add, plane_of(field, 0, k), each_fine(ahead, k)), k)

        drain(leave.at[2], corr_in)
        drain(leave.at[1], rates.at[away])


def hand_out_kernel(end_ref, next_ref, end_out, next_out, sems):
    copies = [
        pltpu.make_async_copy(end_ref, end_out, sems.at[0]),
        pltpu.make_async_copy(next_ref, next_out, sems.at[1]),
    ]
    for copy in copies:
        copy.start()
    for copy in copies:
        copy.wait()


def hand_out(end, following):
    return pl.pallas_call(
        hand_out_kernel,
        out_shape=[jax.ShapeDtypeStruct(end.shape, end.dtype)] * 2,
        in_specs=[pl.BlockSpec(memory_space=pltpu.VMEM)] * 2,
        out_specs=[pl.BlockSpec(memory_space=pl.ANY)] * 2,
        scratch_shapes=[pltpu.SemaphoreType.DMA((2,))],
    )(*(pltpu.with_memory_space_constraint(x, pltpu.VMEM) for x in (end, following)))


def solution(mesh):
    slabs, parts = mesh.shape["tm"], mesh.shape["gz"]

    def per_device(starts, cell_rates):
        depth, rows, lanes = cell_rates.shape
        layers = depth * parts
        groups = slabs // 2
        vectors = rows // SUBLANES
        fine = (vectors, SUBLANES, lanes)
        coarse = (vectors // 2, SUBLANES, lanes)
        packed = (layers // 4, *coarse)
        lead = (depth // 2, *coarse)
        aside = max(parts - 1, 1)
        dma = pltpu.SemaphoreType.DMA

        def vmem(*shape):
            return pltpu.VMEM(shape, jnp.float32)

        ends = pl.pallas_call(
            functools.partial(kernel, slabs, parts),
            out_shape=[pltpu.VMEM(starts.shape, jnp.float32)] * 2,
            in_specs=[pl.BlockSpec(memory_space=pl.ANY)] * 2,
            out_specs=[pl.BlockSpec(memory_space=pltpu.VMEM)] * 2,
            scratch_shapes=[
                vmem(2, layers, rows, lanes),
                vmem(layers, rows, lanes),
                vmem(layers, *fine),
                vmem(layers, *fine),
                vmem(2, 2, layers, *fine),
                vmem(2, layers, *fine),
                vmem(parts, 2, *packed),
                vmem(2, aside, *packed),
                vmem(groups, *packed),
                vmem(groups, parts, *packed),
                vmem(parts, *lead),
                vmem(parts, *lead),
                vmem(2, *lead),
                vmem(2, *lead),
                vmem(depth, *fine),
                vmem(aside, depth, *fine),
                vmem(*packed),
                vmem(layers, rows, lanes),
                pltpu.SemaphoreType.REGULAR((4,)),
                dma((9,)),
                dma((8 + groups,)),
            ],
            compiler_params=pltpu.CompilerParams(collective_id=0, has_side_effects=True),
        )(starts, cell_rates)
        return hand_out(*ends)

    return jax.shard_map(
        per_device,
        mesh=mesh,
        in_specs=(P("tm", "gz", None, None), P("gz", None, None)),
        out_specs=(P("tm", "gz", None, None), P("tm", "gz", None, None)),
        check_vma=False,
    )
```

```python
import functools

import jax
import jax.numpy as jnp
from jax import lax
from jax.experimental import pallas as pl
from jax.experimental.pallas import tpu as pltpu
from jax.sharding import PartitionSpec as P

MESH = pl.DeviceIdType.MESH
FINE = 4
SUBLANES = 8

fine_along_z = (0.1, 0.12)
fine_along_x = (0.15, 0.12)
fine_along_y = (0.2, 0.12)
coarse_along_z = (0.2, 0.25)
coarse_along_x = (0.3, 0.25)
coarse_along_y = (0.4, 0.25)


def blend(behind, middle, beyond, along):
    courant, diffuse = along
    center = 1.0 - 2.0 * diffuse
    before, after = (diffuse + 0.5 * courant) / center, (diffuse - 0.5 * courant) / center
    if middle is None:
        return before * behind if beyond is None else after * beyond
    if behind is None:
        return middle if beyond is None else middle + after * beyond
    if beyond is None:
        return middle + before * behind
    return middle + (before * behind + after * beyond)


def centers(*alongs):
    product = 1.0
    for _, diffuse in alongs:
        product *= 1.0 - 2.0 * diffuse
    return product


def turned(values, by, dim):
    return pltpu.roll(values, by % values.shape[dim], dim)


def lane_filtered(values, by, along):
    return blend(turned(values, by, 1), values, turned(values, -by, 1), along)


def row_filtered(plane, along):
    ring = (turned(plane[-1], 1, 0), *plane, turned(plane[0], -1, 0))
    return tuple(blend(*ring[j : j + 3], along) for j in range(len(plane)))


def each(f, *planes):
    return tuple(f(*vectors) for vectors in zip(*planes))


def kernel(
    slabs, parts, starts_ref, rates_ref, end_ref, next_ref,
    state, rates, pull, keep, mixed, field, shares, shares_in, sums, wraps, crown, crown_in,
    heads, heads_in, corr_in, parts_in, base, raw_in,
    ready, leave, arrive,
):
    depth, rows, lanes = rates_ref.shape
    layers = depth * parts
    groups = slabs // 2
    coarse_layers, coarse_rows, coarse_depth = layers // 2, rows // 2, depth // 2
    half = coarse_layers // 2
    vectors = rows // SUBLANES
    coarse_vectors = vectors // 2
    me, part = lax.axis_index("tm"), lax.axis_index("gz")
    group, place = me // 2, lax.rem(me, 2)
    leads, helps = place == 1, place == 0
    last = group == groups - 1
    direct, proxy = (group == 0) & (part == 0), (group == 0) & (part > 0)

    def block(r):
        return pl.ds(r % parts * depth, depth)

    own = block(0)
    rate_load = pltpu.make_async_copy(rates_ref, rates.at[own], leave.at[5])
    state_load = pltpu.make_async_copy(starts_ref.at[0], state.at[place, own], leave.at[6])
    rate_load.start()
    state_load.start()

    def leader(g, i):
        return {"tm": 2 * g + 1, "gz": lax.rem(part + i, parts)}

    def helper(g, i):
        return {"tm": 2 * g, "gz": lax.rem(part + i, parts)}

    def signal(sem, peer):
        pl.semaphore_signal(sem, inc=1, device_id=peer, device_id_type=MESH)

    def remote(src, dst, send_sem, recv_sem, peer):
        return pltpu.make_async_remote_copy(
            src_ref=src, dst_ref=dst, send_sem=send_sem, recv_sem=recv_sem,
            device_id=peer, device_id_type=MESH,
        )

    others = range(1, parts)
    barrier = pltpu.get_barrier_semaphore()
    here, near_open, far_open = (ready.at[n] for n in range(3))
    line = 8

    @pl.when(leads)
    def _():
        for i in others:
            signal(barrier, leader(group, i))
        signal(barrier, helper(group, 0))
        for j in range(1, groups):
            @pl.when(group + j < groups)
            def _():
                signal(barrier, leader(group + j, 0))

        @pl.when(proxy)
        def _():
            for j in range(1, groups):
                for i in others:
                    signal(barrier, leader(j, i))

    @pl.when(helps)
    def _():
        for i in others:
            signal(barrier, helper(group, i))

        @pl.when(direct)
        def _():
            for j in range(1, groups):
                for i in range(parts):
                    signal(barrier, leader(j, i))

    earlier = group + jnp.where(group > 0, parts - jnp.where(part > 0, 1, 0), 0)
    pl.semaphore_wait(barrier, jnp.where(leads, parts - 1 + earlier, parts))

    def drain(sem, ref):
        pltpu.make_async_copy(ref, ref, sem).wait()

    def raw_copy():
        piece = state.at[0, own]
        return remote(piece, piece, leave.at[0], arrive.at[0], leader(group, 0))

    def rate_copy(i):
        return remote(
            rates.at[own], rates.at[block(parts - i)],
            leave.at[0], arrive.at[1], leader(group, i),
        )

    def hand_copy(i):
        piece = rates.at[block(i)]
        return remote(piece, piece, leave.at[1], arrive.at[1], helper(group, 0))

    def side_copy(i):
        return remote(
            state.at[0, own], state.at[0, block(parts - i)], leave.at[1], arrive.at[2], helper(group, i)
        )

    def offset_to(q):
        return lax.rem(q + parts - part, parts)

    def home(i):
        q = lax.rem(part + i, parts)
        return {"tm": jnp.where(q == 0, 0, 1), "gz": q}

    def raw_next(i, send_sem, peer):
        r = lax.rem(parts - i, parts)
        return remote(state.at[1, own], raw_in.at[pl.ds(r * depth, depth)], send_sem, arrive.at[7], peer)

    def next_copy():
        return raw_next(0, leave.at[2], helper(group + 1, 0))

    def across_copy(i):
        return remote(raw_in.at[own], raw_in.at[block(parts - i)], leave.at[3], arrive.at[0], helper(group, i))

    def round_copy(i):
        return raw_next(i, leave.at[2], home(i))

    def forward_copy():
        return remote(raw_in, raw_in, leave.at[3], arrive.at[7], helper(0, 0))

    def wrap_copy(i):
        return remote(
            shares.at[i, 0], wraps.at[group, lax.rem(parts - i, parts)], leave.at[3], arrive.at[line + group],
            home(i),
        )

    def first_copy():
        return remote(sums.at[0], wraps.at[0, 0], leave.at[3], arrive.at[line], helper(0, 0))

    def crown_copy(i):
        return remote(
            crown.at[i], crown_in.at[lax.rem(parts - i, parts)], leave.at[3], arrive.at[line + group],
            home(i),
        )

    def share_copy(i, n):
        return remote(
            shares.at[i, n], shares_in.at[n, parts - i - 1], leave.at[4 if n == 0 else 8],
            arrive.at[3 if n == 0 else 6], leader(group, i),
        )

    def sum_copy(j):
        piece = sums.at[group]
        return remote(piece, piece, leave.at[7], arrive.at[line + group], leader(group + j, 0))

    def part_copy(i):
        return remote(
            field.at[1, block(i)], parts_in.at[parts - i - 1], leave.at[5], arrive.at[4], leader(group, i)
        )

    def corr_copy():
        return remote(field.at[0, own], corr_in, leave.at[2], arrive.at[5], leader(group, 0))

    def head_copy():
        return remote(heads, heads_in, leave.at[6], arrive.at[3], helper(group, 0))

    even = lax.rem(lax.broadcasted_iota(jnp.int32, (SUBLANES, lanes), 1), 2) == 0
    fine_center = centers(fine_along_y, fine_along_x, fine_along_z)
    coarse_center = centers(coarse_along_y, coarse_along_x, coarse_along_z)
    strides = [pl.ds(j, SUBLANES, stride=vectors) for j in range(vectors)]

    def raw_plane(ref, *where):
        return tuple(ref[(*where, stride)] for stride in strides)

    def plane_of(ref, *where):
        return tuple(ref[(*where, j)] for j in range(ref.shape[-3]))

    def put(ref, plane, *where):
        for j, vector in enumerate(plane):
            ref[(*where, j)] = vector

    def prepare(ks):
        for k in ks:
            rate = raw_plane(rates, k)
            put(pull, each(lambda r: r * fine_center, rate), k)
            put(keep, each(lambda r: 1.0 - r, rate), k)

    def restricted(upper, lower):
        merged = each(jnp.add, upper, lower)
        averages = []
        for j in range(coarse_vectors):
            total = merged[2 * j] + merged[2 * j + 1]
            pair_sum = total + jnp.where(even, turned(total, -1, 1), turned(total, 1, 1))
            averages.append(pair_sum * 0.125)
        return tuple(averages)

    def restricted_and_filtered(upper, lower, guess):
        merged = each(jnp.add, upper, lower)
        total = tuple(merged[2 * j] + merged[2 * j + 1] for j in range(coarse_vectors))
        if guess is not None:
            total = each(lambda t, g: t - 4.0 * g, total, guess)
        total = each(lambda t: t * 0.125, total)
        t = shifted(total)

        def pair(n):
            return each(lambda here, a, b: here + jnp.where(even, a, b), t[n], t[n - 1], t[n + 1])

        here = pair(0)
        sides = each(lambda *v: blend(*v, coarse_along_y), pair(2), here, pair(-2))
        return here, row_filtered(sides, coarse_along_x)

    def raw_restricted(ref, k, *lead):
        return restricted(raw_plane(ref, *lead, 2 * k), raw_plane(ref, *lead, 2 * k + 1))

    def field_restricted(s, k):
        return restricted(plane_of(field, s, 2 * k), plane_of(field, s, 2 * k + 1))

    def coarse_rates(ks):
        weights = {k: raw_restricted(rates, k) for k in ks}
        return (
            {k: each(lambda v: v * coarse_center, w) for k, w in weights.items()},
            {k: each(lambda v: 1.0 - v, w) for k, w in weights.items()},
        )

    def stepped(trio, held, pulls, keeps, along):
        behind, middle, beyond = trio
        if middle is None and behind is not None and beyond is not None:
            deep = each(
                lambda b, f: blend(b, None, None, along) + blend(None, None, f, along), behind, beyond
            )
        else:
            there = [p for p in trio if p is not None]

            def mix(*given):
                given = iter(given)
                return blend(*(None if p is None else next(given) for p in trio), along)

            deep = each(mix, *there)
        if held is None:
            return each(jnp.multiply, pulls, deep)
        return each(lambda p, d, q, h: p * d + q * h, pulls, deep, keeps, held)

    def coarse_filtered(plane):
        return row_filtered(each(lambda v: lane_filtered(v, 2, coarse_along_y), plane), coarse_along_x)

    def advance(coarse, mixes, pulls, keeps, wanted):
        moved = [None] * coarse_layers
        for k in wanted:
            trio = mixes[k - 1], mixes[k], mixes[(k + 1) % coarse_layers]
            if any(p is not None for p in trio):
                moved[k] = stepped(trio, coarse[k], pulls[k], keeps[k], coarse_along_z)
        return moved

    def all_filtered(coarse):
        return [None if c is None else coarse_filtered(c) for c in coarse]

    def packed(coarse, shift=0):
        def layer(k):
            return coarse[(k + shift) % coarse_layers]

        return [each(lambda a, b: jnp.where(even, a, b), layer(k), layer(k + half)) for k in range(half)]

    def shifted(plane):
        return {n: each(lambda v: turned(v, n, 1), plane) for n in (1, 2, 3, -1, -2, -3)} | {0: plane}

    def mixed_lanes(t, even_by, odd_by):
        trio = [
            t[even_by + n]
            if even_by == odd_by
            else each(lambda a, b: jnp.where(even, a, b), t[even_by + n], t[odd_by + n])
            for n in (2, 0, -2)
        ]
        return trio[1], row_filtered(each(lambda *v: blend(*v, coarse_along_y), *trio), coarse_along_x)

    def advance_packed(coarse, pulls, keeps):
        turns = [shifted(c) for c in coarse]
        planes = [mixed_lanes(t, 0, 0)[1] for t in turns]
        low, high = mixed_lanes(turns[-1], -1, 1)[1], mixed_lanes(turns[0], -1, 1)[1]
        ring = [low] + planes + [high]
        return [
            stepped(ring[k : k + 3], coarse[k], pulls[k], keeps[k], coarse_along_z) for k in range(half)
        ]

    def advance_opened(coarse, pulls, keeps):
        turns = [shifted(c) for c in coarse]

        def opened(k):
            k = k % coarse_layers
            return mixed_lanes(turns[k % half], *((0, 1) if k < half else (-1, 0)))

        ring = [opened(k) for k in range(-1, coarse_depth + 1)]
        return [
            stepped([r[1] for r in ring[k : k + 3]], ring[k + 1][0], pulls[k], keeps[k], coarse_along_z)
            for k in range(coarse_depth)
        ]

    def open_lanes(coarse, k):
        both = coarse[k % half]
        if k < half:
            return each(lambda v: jnp.where(even, v, turned(v, 1, 1)), both)
        return each(lambda v: jnp.where(even, turned(v, -1, 1), v), both)

    def plus(first, second):
        return [
            b if a is None else a if b is None else each(jnp.add, a, b) for a, b in zip(first, second)
        ]

    def packed_in(ref, *where):
        return [plane_of(ref, *where, k) for k in range(half)]

    def grown(ks):
        return sorted({(k + n) % layers for k in ks for n in (-1, 0, 1)})

    def origin(s, k):
        return raw_plane(state, s, k)

    def held_plane(s, turn, k, first):
        return first(s, k) if turn == 0 else plane_of(field, s, k)

    def spread(s, turn, ks, first=origin):
        for k in ks:
            sides = each(lambda v: lane_filtered(v, 1, fine_along_y), held_plane(s, turn, k, first))
            put(mixed, row_filtered(sides, fine_along_x), turn % 2, s, k)

    def settle(s, turn, live, ks, first=origin):
        for k in ks:
            trio = [
                plane_of(mixed, turn % 2, s, n % layers) if n % layers in live else None
                for n in (k - 1, k, k + 1)
            ]
            held = held_plane(s, turn, k, first) if k in live else None
            put(field, stepped(trio, held, plane_of(pull, k), plane_of(keep, k), fine_along_z), s, k)

    own_layers, own_coarse = list(range(depth)), list(range(coarse_depth))
    all_layers, all_coarse = list(range(layers)), list(range(coarse_layers))
    nothing = (jnp.zeros((SUBLANES, lanes), jnp.float32),) * coarse_vectors

    def each_fine(coarse, k):
        return tuple(coarse[k // 2][j // 2] for j in range(vectors))

    def sent_on(s, guess, ks):
        for k in ks:
            if guess[k // 2] is not None:
                put(field, each(jnp.subtract, plane_of(field, s, k), each_fine(guess, k)), s, k)

    def hand_in(ref, plane, k):
        for stride, vector in zip(strides, plane):
            ref[0, k, stride, :] = vector

    @pl.when(leads)
    def _():
        for j in range(2, groups):
            @pl.when(group - j >= 0)
            def _():
                signal(far_open, leader(group - j, 0))

        rate_load.wait()
        for i in others:
            rate_copy(i).start()
        state_load.wait()

        @pl.when(last)
        def _():
            for q in range(parts):
                round_copy(offset_to(q)).start()

        prepare(own_layers)
        lives = [own_layers]
        for _ in range(FINE):
            lives.append(grown(lives[-1]))
        ready_now = [own_layers]
        for turn in range(FINE):
            known = set(ready_now[-1])
            ready_now.append([
                k for k in own_layers
                if all(n % layers in known or n % layers not in lives[turn] for n in (k - 1, k, k + 1))
            ])

        def early(s):
            for turn in range(FINE):
                spread(s, turn, ready_now[turn])
                settle(s, turn, lives[turn], ready_now[turn + 1])

        def late(turn):
            for s in (0, 1):
                spread(s, turn, [k for k in lives[turn] if k not in ready_now[turn]])
            for s in (0, 1):
                settle(
                    s, turn, lives[turn], [k for k in lives[turn + 1] if k not in ready_now[turn + 1]]
                )

        def begin_of(s):
            begin = [raw_restricted(state, k, s) for k in own_coarse]
            begin += [None] * (coarse_layers - coarse_depth)
            return begin, all_filtered(begin)

        early(1)
        begins = {1: begin_of(1)}
        own_pulls, own_keeps = coarse_rates(own_coarse)
        pl.semaphore_wait(here, 1)

        @pl.when(group > 0)
        def _():
            signal(near_open, leader(group - 1, 0))

        raw_copy().wait_recv()
        early(0)
        begins[0] = begin_of(0)
        drain(arrive.at[1], rates.at[pl.ds(0, depth * (parts - 1))])
        for i in others:
            hand_copy(i).start()

        @pl.when(~last)
        def _():
            pl.semaphore_wait(near_open, 1)
            next_copy().start()

        prepare([k for k in all_layers if k not in own_layers])
        for turn in range(FINE):
            late(turn)
        live = lives[-1]
        pulls, keeps = coarse_rates(all_coarse[coarse_depth:])
        pulls, keeps = own_pulls | pulls, own_keeps | keeps
        guesses = []
        for s, gate in ((0, jnp.where(group > 0, 1.0, 0.0)), (1, None)):
            guess = advance(*begins[s], pulls, keeps, all_coarse)
            if gate is not None:
                guess = [g if g is None else each(lambda v: gate * v, g) for g in guess]
            guesses.append(guess)
        for s in (0, 1):
            for k in all_layers:
                if k not in live:
                    put(field, (jnp.zeros((SUBLANES, lanes), jnp.float32),) * vectors, s, k)

        def fine_of(s, k):
            return plane_of(field, s, 2 * k), plane_of(field, s, 2 * k + 1)

        def zero_guess(s, k):
            return guesses[s][k] if guesses[s][k] is not None else nothing

        both = [
            restricted_and_filtered(*fine_of(0, k), guesses[0][k])
            if 2 * k in live
            else (each(jnp.negative, zero_guess(0, k)), coarse_filtered(each(jnp.negative, zero_guess(0, k))))
            for k in all_coarse
        ]
        term = [b[0] for b in both]
        after = [
            each(jnp.subtract, restricted(*fine_of(1, k)) if 2 * k in live else nothing, zero_guess(1, k))
            for k in all_coarse
        ]
        run = plus(advance(term, [b[1] for b in both], pulls, keeps, all_coarse), after)
        for i in range(parts):
            shift = i * coarse_depth
            for k, c in enumerate(packed(run, shift)):
                put(shares, c, i, 0, k)
            for k in own_coarse:
                put(crown, run[(k + shift) % coarse_layers], i, k)

        @pl.when(last)
        def _():
            for q in range(parts):
                crown_copy(offset_to(q)).start()

        @pl.when(~last & (group > 0))
        def _():
            for q in range(parts):
                wrap_copy(offset_to(q)).start()

        for i in others:
            share_copy(i, 0).start()
        for i in range(parts):
            for k, c in enumerate(packed(term, i * coarse_depth)):
                put(shares, c, i, 1, k)
        sent_on(1, guesses[1], all_layers)

        @pl.when(group == 0)
        def _():
            for i in others:
                part_copy(i).start()
                share_copy(i, 1).start()

        @pl.when(group + 2 < groups)
        def _():
            pl.semaphore_wait(far_open, groups - 2 - group)

        drain(arrive.at[3], shares_in.at[0])
        total = packed_in(shares, 0, 0)
        for r in others:
            total = plus(total, packed_in(shares_in, 0, r - 1))
        for k in range(half):
            put(sums, total[k], group, k)
        for j in reversed(range(1, groups)):
            @pl.when(group + j < groups)
            def _():
                sum_copy(j).start()

        @pl.when(direct)
        def _():
            first_copy().start()

        @pl.when(group > 0)
        def _():
            for i in others:
                share_copy(i, 1).start()

        packed_pulls, packed_keeps = packed(pulls), packed(keeps)

        def twice(coarse):
            for _ in range(2):
                coarse = advance_packed(coarse, packed_pulls, packed_keeps)
            return coarse

        @pl.when(group > 0)
        def _():
            drain(arrive.at[line], sums.at[0])
            for i in others:
                part_copy(i).start()

        @pl.when(group == 0)
        def _():
            for k in range(half):
                put(base, nothing, k)

        @pl.when(group > 0)
        def _():
            def pass_group(index, coarse):
                coarse = twice(coarse)
                drain(arrive.at[line + index], sums.at[index])
                return plus(coarse, packed_in(sums, index))

            coarse = lax.fori_loop(1, group, pass_group, packed_in(sums, 0))
            for k in range(half):
                put(base, coarse[k], k)

        coarse = packed_in(base)
        ahead = advance_opened(coarse, pulls, keeps)

        @pl.when(group > 0)
        def _():
            for k in own_coarse:
                put(heads, open_lanes(coarse, k), 0, k)
                put(heads, ahead[k], 1, k)
            head_copy().start()

        drain(arrive.at[6], shares_in.at[1])
        middle = packed_in(shares, 0, 1)
        for r in others:
            middle = plus(middle, packed_in(shares_in, 1, r - 1))
        finish = advance_opened(
            plus(advance_packed(coarse, packed_pulls, packed_keeps), middle), pulls, keeps
        )
        corr_copy().wait_recv()
        drain(arrive.at[4], parts_in)
        for k in own_layers:
            hand_in(next_ref, each(jnp.add, plane_of(corr_in, k), each_fine(ahead, k)), k)
            held = plane_of(field, 1, k)
            for r in others:
                held = each(jnp.add, held, plane_of(parts_in, r - 1, k))
            hand_in(end_ref, each(jnp.add, held, each_fine(finish, k)), k)
        away = pl.ds(0, depth * (parts - 1))
        drain(leave.at[0], rates.at[away])
        drain(leave.at[1], rates.at[away])
        @pl.when(~last)
        def _():
            drain(leave.at[2], raw_in.at[own])

        drain(leave.at[4], shares_in.at[0])
        drain(leave.at[8], shares_in.at[1])
        drain(leave.at[5], parts_in)
        for j in range(1, groups):
            @pl.when(groups - 1 - group == j)
            def _():
                drain(leave.at[7], sums.at[pl.ds(0, j)])

        @pl.when(last)
        def _():
            drain(leave.at[2], raw_in)
            drain(leave.at[3], crown_in)

        @pl.when(~last & (group > 0))
        def _():
            drain(leave.at[3], wraps.at[0])

        @pl.when(direct)
        def _():
            drain(leave.at[3], sums.at[0])

        @pl.when(proxy)
        def _():
            drain(arrive.at[7], raw_in)
            forward_copy().start()

            def pass_group(index, coarse):
                coarse = twice(coarse)
                drain(arrive.at[line + index], wraps.at[index])
                for r in range(parts):
                    coarse = plus(coarse, packed_in(wraps, index, r))
                return coarse

            coarse = lax.fori_loop(1, groups - 1, pass_group, packed_in(sums, 0))
            coarse = advance_packed(coarse, packed_pulls, packed_keeps)
            coarse = advance_opened(coarse, pulls, keeps)
            drain(arrive.at[line + groups - 1], crown_in)
            for k in own_coarse:
                following = coarse[k]
                for r in range(parts):
                    following = each(jnp.add, following, plane_of(crown_in, r, k))
                put(heads, following, 0, k)
                put(heads, nothing, 1, k)
            head_copy().start()
            drain(leave.at[3], raw_in)

        @pl.when(~direct)
        def _():
            drain(leave.at[6], heads)

    @pl.when(helps)
    def _():
        signal(here, leader(group, 0))
        state_load.wait()
        raw_copy().start()
        rate_load.wait()
        prepare(own_layers)
        raw_copy().wait_send()
        for i in others:
            side_copy(i).start()
        away = pl.ds(0, depth * (parts - 1))
        drain(arrive.at[2], rates.at[away])
        drain(arrive.at[1], rates.at[away])
        prepare([k for k in all_layers if k not in own_layers])
        pulls, keeps = coarse_rates(all_coarse)

        def solve(s, gate):
            def first(s, k):
                return raw_plane(state, 0, k) if s == 0 else raw_plane(raw_in, k)

            begin = [restricted(first(s, 2 * k), first(s, 2 * k + 1)) for k in all_coarse]
            guess = advance(begin, all_filtered(begin), pulls, keeps, own_coarse)
            if gate is not None:
                guess = [g if g is None else each(lambda v: gate * v, g) for g in guess]
            wanted = [own_layers]
            for _ in range(1, FINE):
                wanted.append(grown(wanted[-1]))
            for turn in range(FINE):
                reach = wanted[FINE - 1 - turn]
                spread(s, turn, grown(reach), first)
                settle(s, turn, all_layers, reach, first)
            sent_on(s, guess, own_layers)

        solve(0, jnp.where(group > 0, 1.0, 0.0))
        corr_copy().start()
        packed_pulls, packed_keeps = packed(pulls), packed(keeps)

        def arrived(index):
            drain(arrive.at[line + index], wraps.at[index])

        def with_arrived(coarse, index):
            for r in range(parts):
                coarse = plus(coarse, packed_in(wraps, index, r))
            return coarse

        def twice(coarse):
            for _ in range(2):
                coarse = advance_packed(coarse, packed_pulls, packed_keeps)
            return coarse

        def second_solve():
            solve(1, None)
            before = [field_restricted(1, k) for k in own_coarse]
            sent_on(1, before, own_layers)

        @pl.when(direct)
        def _():
            for k in own_layers:
                hand_in(end_ref, plane_of(field, 0, k), k)
            drain(arrive.at[line], wraps.at[0, 0])
            coarse = twice(packed_in(wraps, 0, 0))
            drain(arrive.at[7], raw_in)
            second_solve()
            for index in range(1, groups - 1):
                arrived(index)
                coarse = with_arrived(coarse, index)
                if index < groups - 2:
                    coarse = twice(coarse)
            coarse = advance_packed(coarse, packed_pulls, packed_keeps)
            coarse = advance_opened(coarse, pulls, keeps)
            for k in own_layers:
                put(field, each(jnp.add, plane_of(field, 1, k), each_fine(coarse, k)), 1, k)
            drain(arrive.at[line + groups - 1], crown_in)
            for k in own_layers:
                following = plane_of(field, 1, k)
                for r in range(parts):
                    offset = each_fine([plane_of(crown_in, r, c) for c in own_coarse], k)
                    following = each(jnp.add, following, offset)
                hand_in(next_ref, following, k)

        @pl.when(proxy)
        def _():
            drain(arrive.at[7], raw_in)

        @pl.when(group > 0)
        def _():
            drain(arrive.at[7], raw_in.at[own])
            for i in others:
                across_copy(i).start()
            drain(arrive.at[0], raw_in.at[away])

        @pl.when(~direct)
        def _():
            second_solve()
            head_copy().wait_recv()
            for k in own_layers:
                coarse, ahead = ([plane_of(heads_in, n, c) for c in own_coarse] for n in range(2))
                hand_in(next_ref, each(jnp.add, plane_of(field, 1, k), each_fine(coarse, k)), k)
                hand_in(end_ref, each(jnp.add, plane_of(field, 0, k), each_fine(ahead, k)), k)

        @pl.when(group > 0)
        def _():
            drain(leave.at[3], raw_in.at[away])

        drain(leave.at[2], corr_in)
        drain(leave.at[1], rates.at[away])


def hand_out_kernel(end_ref, next_ref, end_out, next_out, sems):
    copies = [
        pltpu.make_async_copy(end_ref, end_out, sems.at[0]),
        pltpu.make_async_copy(next_ref, next_out, sems.at[1]),
    ]
    for copy in copies:
        copy.start()
    for copy in copies:
        copy.wait()


def hand_out(end, following):
    return pl.pallas_call(
        hand_out_kernel,
        out_shape=[jax.ShapeDtypeStruct(end.shape, end.dtype)] * 2,
        in_specs=[pl.BlockSpec(memory_space=pltpu.VMEM)] * 2,
        out_specs=[pl.BlockSpec(memory_space=pl.ANY)] * 2,
        scratch_shapes=[pltpu.SemaphoreType.DMA((2,))],
    )(*(pltpu.with_memory_space_constraint(x, pltpu.VMEM) for x in (end, following)))


def solution(mesh):
    slabs, parts = mesh.shape["tm"], mesh.shape["gz"]

    def per_device(starts, cell_rates):
        depth, rows, lanes = cell_rates.shape
        layers = depth * parts
        groups = slabs // 2
        vectors = rows // SUBLANES
        fine = (vectors, SUBLANES, lanes)
        coarse = (vectors // 2, SUBLANES, lanes)
        packed = (layers // 4, *coarse)
        lead = (depth // 2, *coarse)
        aside = max(parts - 1, 1)
        dma = pltpu.SemaphoreType.DMA

        def vmem(*shape):
            return pltpu.VMEM(shape, jnp.float32)

        ends = pl.pallas_call(
            functools.partial(kernel, slabs, parts),
            out_shape=[pltpu.VMEM(starts.shape, jnp.float32)] * 2,
            in_specs=[pl.BlockSpec(memory_space=pl.ANY)] * 2,
            out_specs=[pl.BlockSpec(memory_space=pltpu.VMEM)] * 2,
            scratch_shapes=[
                vmem(2, layers, rows, lanes),
                vmem(layers, rows, lanes),
                vmem(layers, *fine),
                vmem(layers, *fine),
                vmem(2, 2, layers, *fine),
                vmem(2, layers, *fine),
                vmem(parts, 2, *packed),
                vmem(2, aside, *packed),
                vmem(groups, *packed),
                vmem(groups, parts, *packed),
                vmem(parts, *lead),
                vmem(parts, *lead),
                vmem(2, *lead),
                vmem(2, *lead),
                vmem(depth, *fine),
                vmem(aside, depth, *fine),
                vmem(*packed),
                vmem(layers, rows, lanes),
                pltpu.SemaphoreType.REGULAR((3,)),
                dma((9,)),
                dma((8 + groups,)),
            ],
            compiler_params=pltpu.CompilerParams(collective_id=0, has_side_effects=True),
        )(starts, cell_rates)
        return hand_out(*ends)

    return jax.shard_map(
        per_device,
        mesh=mesh,
        in_specs=(P("tm", "gz", None, None), P("gz", None, None)),
        out_specs=(P("tm", "gz", None, None), P("tm", "gz", None, None)),
        check_vma=False,
    )
```

```python
import functools

import jax
import jax.numpy as jnp
from jax import lax
from jax.experimental import pallas as pl
from jax.experimental.pallas import tpu as pltpu
from jax.sharding import PartitionSpec as P

MESH = pl.DeviceIdType.MESH
FINE = 4
SUBLANES = 8

fine_along_z = (0.1, 0.12)
fine_along_x = (0.15, 0.12)
fine_along_y = (0.2, 0.12)
coarse_along_z = (0.2, 0.25)
coarse_along_x = (0.3, 0.25)
coarse_along_y = (0.4, 0.25)


def blend(behind, middle, beyond, along):
    courant, diffuse = along
    center = 1.0 - 2.0 * diffuse
    before, after = (diffuse + 0.5 * courant) / center, (diffuse - 0.5 * courant) / center
    if middle is None:
        return before * behind if beyond is None else after * beyond
    if behind is None:
        return middle if beyond is None else middle + after * beyond
    if beyond is None:
        return middle + before * behind
    return middle + (before * behind + after * beyond)


def centers(*alongs):
    product = 1.0
    for _, diffuse in alongs:
        product *= 1.0 - 2.0 * diffuse
    return product


def turned(values, by, dim):
    return pltpu.roll(values, by % values.shape[dim], dim)


def lane_filtered(values, by, along):
    return blend(turned(values, by, 1), values, turned(values, -by, 1), along)


def row_filtered(plane, along):
    ring = (turned(plane[-1], 1, 0), *plane, turned(plane[0], -1, 0))
    return tuple(blend(*ring[j : j + 3], along) for j in range(len(plane)))


def each(f, *planes):
    return tuple(f(*vectors) for vectors in zip(*planes))


def kernel(
    slabs, parts, starts_ref, rates_ref, end_ref, next_ref,
    state, rates, pull, keep, mixed, field, shares, shares_in, sums, wraps, crown, crown_in,
    heads, heads_in, corr_in, parts_in, base, raw_in,
    ready, leave, arrive,
):
    depth, rows, lanes = rates_ref.shape
    layers = depth * parts
    groups = slabs // 2
    coarse_layers, coarse_rows, coarse_depth = layers // 2, rows // 2, depth // 2
    half = coarse_layers // 2
    vectors = rows // SUBLANES
    coarse_vectors = vectors // 2
    me, part = lax.axis_index("tm"), lax.axis_index("gz")
    group, place = me // 2, lax.rem(me, 2)
    leads, helps = place == 1, place == 0
    last = group == groups - 1
    direct, proxy = (group == 0) & (part == 0), (group == 0) & (part > 0)

    def block(r):
        return pl.ds(r % parts * depth, depth)

    own = block(0)
    rate_load = pltpu.make_async_copy(rates_ref, rates.at[own], leave.at[5])
    state_load = pltpu.make_async_copy(starts_ref.at[0], state.at[place, own], leave.at[6])
    def leader(g, i):
        return {"tm": 2 * g + 1, "gz": lax.rem(part + i, parts)}

    def helper(g, i):
        return {"tm": 2 * g, "gz": lax.rem(part + i, parts)}

    def signal(sem, peer):
        pl.semaphore_signal(sem, inc=1, device_id=peer, device_id_type=MESH)

    def remote(src, dst, send_sem, recv_sem, peer):
        return pltpu.make_async_remote_copy(
            src_ref=src, dst_ref=dst, send_sem=send_sem, recv_sem=recv_sem,
            device_id=peer, device_id_type=MESH,
        )

    others = range(1, parts)
    barrier = pltpu.get_barrier_semaphore()
    here, near_open, far_open = (ready.at[n] for n in range(3))
    line = 8

    @pl.when(leads)
    def _():
        for i in others:
            signal(barrier, leader(group, i))
        rate_load.start()
        state_load.start()
        signal(barrier, helper(group, 0))
        for j in range(1, groups):
            @pl.when(group + j < groups)
            def _():
                signal(barrier, leader(group + j, 0))

        @pl.when(proxy)
        def _():
            for j in range(1, groups):
                for i in others:
                    signal(barrier, leader(j, i))

    @pl.when(helps)
    def _():
        state_load.start()
        rate_load.start()
        for i in others:
            signal(barrier, helper(group, i))

        @pl.when(direct)
        def _():
            for j in range(1, groups):
                for i in range(parts):
                    signal(barrier, leader(j, i))

    earlier = group + jnp.where(group > 0, parts - jnp.where(part > 0, 1, 0), 0)
    pl.semaphore_wait(barrier, jnp.where(leads, parts - 1 + earlier, parts))

    def drain(sem, ref):
        pltpu.make_async_copy(ref, ref, sem).wait()

    def raw_copy():
        piece = state.at[0, own]
        return remote(piece, piece, leave.at[0], arrive.at[0], leader(group, 0))

    def rate_copy(i):
        return remote(
            rates.at[own], rates.at[block(parts - i)],
            leave.at[0], arrive.at[1], leader(group, i),
        )

    def hand_copy(i):
        piece = rates.at[block(i)]
        return remote(piece, piece, leave.at[1], arrive.at[1], helper(group, 0))

    def side_copy(i):
        return remote(
            state.at[0, own], state.at[0, block(parts - i)], leave.at[1], arrive.at[2], helper(group, i)
        )

    def offset_to(q):
        return lax.rem(q + parts - part, parts)

    def home(i):
        q = lax.rem(part + i, parts)
        return {"tm": jnp.where(q == 0, 0, 1), "gz": q}

    def raw_next(i, send_sem, peer):
        r = lax.rem(parts - i, parts)
        return remote(state.at[1, own], raw_in.at[pl.ds(r * depth, depth)], send_sem, arrive.at[7], peer)

    def next_copy():
        return raw_next(0, leave.at[2], helper(group + 1, 0))

    def across_copy(i):
        return remote(raw_in.at[own], raw_in.at[block(parts - i)], leave.at[3], arrive.at[0], helper(group, i))

    def round_copy(i):
        return raw_next(i, leave.at[2], home(i))

    def forward_copy():
        return remote(raw_in, raw_in, leave.at[3], arrive.at[7], helper(0, 0))

    def wrap_copy(i):
        return remote(
            shares.at[i, 0], wraps.at[group, lax.rem(parts - i, parts)], leave.at[3], arrive.at[line + group],
            home(i),
        )

    def first_copy():
        return remote(sums.at[0], wraps.at[0, 0], leave.at[3], arrive.at[line], helper(0, 0))

    def crown_copy(i):
        return remote(
            crown.at[i], crown_in.at[lax.rem(parts - i, parts)], leave.at[3], arrive.at[line + group],
            home(i),
        )

    def share_copy(i, n):
        return remote(
            shares.at[i, n], shares_in.at[n, parts - i - 1], leave.at[4 if n == 0 else 8],
            arrive.at[3 if n == 0 else 6], leader(group, i),
        )

    def sum_copy(j):
        piece = sums.at[group]
        return remote(piece, piece, leave.at[7], arrive.at[line + group], leader(group + j, 0))

    def part_copy(i):
        return remote(
            field.at[1, block(i)], parts_in.at[parts - i - 1], leave.at[5], arrive.at[4], leader(group, i)
        )

    def corr_copy():
        return remote(field.at[0, own], corr_in, leave.at[2], arrive.at[5], leader(group, 0))

    def head_copy():
        return remote(heads, heads_in, leave.at[6], arrive.at[3], helper(group, 0))

    even = lax.rem(lax.broadcasted_iota(jnp.int32, (SUBLANES, lanes), 1), 2) == 0
    fine_center = centers(fine_along_y, fine_along_x, fine_along_z)
    coarse_center = centers(coarse_along_y, coarse_along_x, coarse_along_z)
    strides = [pl.ds(j, SUBLANES, stride=vectors) for j in range(vectors)]

    def raw_plane(ref, *where):
        return tuple(ref[(*where, stride)] for stride in strides)

    def plane_of(ref, *where):
        return tuple(ref[(*where, j)] for j in range(ref.shape[-3]))

    def put(ref, plane, *where):
        for j, vector in enumerate(plane):
            ref[(*where, j)] = vector

    def prepare(ks):
        for k in ks:
            rate = raw_plane(rates, k)
            put(pull, each(lambda r: r * fine_center, rate), k)
            put(keep, each(lambda r: 1.0 - r, rate), k)

    def restricted(upper, lower):
        merged = each(jnp.add, upper, lower)
        averages = []
        for j in range(coarse_vectors):
            total = merged[2 * j] + merged[2 * j + 1]
            pair_sum = total + jnp.where(even, turned(total, -1, 1), turned(total, 1, 1))
            averages.append(pair_sum * 0.125)
        return tuple(averages)

    def restricted_and_filtered(upper, lower, guess):
        merged = each(jnp.add, upper, lower)
        total = tuple(merged[2 * j] + merged[2 * j + 1] for j in range(coarse_vectors))
        if guess is not None:
            total = each(lambda t, g: t - 4.0 * g, total, guess)
        total = each(lambda t: t * 0.125, total)
        t = shifted(total)

        def pair(n):
            return each(lambda here, a, b: here + jnp.where(even, a, b), t[n], t[n - 1], t[n + 1])

        here = pair(0)
        sides = each(lambda *v: blend(*v, coarse_along_y), pair(2), here, pair(-2))
        return here, row_filtered(sides, coarse_along_x)

    def raw_restricted(ref, k, *lead):
        return restricted(raw_plane(ref, *lead, 2 * k), raw_plane(ref, *lead, 2 * k + 1))

    def field_restricted(s, k):
        return restricted(plane_of(field, s, 2 * k), plane_of(field, s, 2 * k + 1))

    def coarse_rates(ks):
        weights = {k: raw_restricted(rates, k) for k in ks}
        return (
            {k: each(lambda v: v * coarse_center, w) for k, w in weights.items()},
            {k: each(lambda v: 1.0 - v, w) for k, w in weights.items()},
        )

    def stepped(trio, held, pulls, keeps, along):
        behind, middle, beyond = trio
        if middle is None and behind is not None and beyond is not None:
            deep = each(
                lambda b, f: blend(b, None, None, along) + blend(None, None, f, along), behind, beyond
            )
        else:
            there = [p for p in trio if p is not None]

            def mix(*given):
                given = iter(given)
                return blend(*(None if p is None else next(given) for p in trio), along)

            deep = each(mix, *there)
        if held is None:
            return each(jnp.multiply, pulls, deep)
        return each(lambda p, d, q, h: p * d + q * h, pulls, deep, keeps, held)

    def coarse_filtered(plane):
        return row_filtered(each(lambda v: lane_filtered(v, 2, coarse_along_y), plane), coarse_along_x)

    def advance(coarse, mixes, pulls, keeps, wanted):
        moved = [None] * coarse_layers
        for k in wanted:
            trio = mixes[k - 1], mixes[k], mixes[(k + 1) % coarse_layers]
            if any(p is not None for p in trio):
                moved[k] = stepped(trio, coarse[k], pulls[k], keeps[k], coarse_along_z)
        return moved

    def all_filtered(coarse):
        return [None if c is None else coarse_filtered(c) for c in coarse]

    def packed(coarse, shift=0):
        def layer(k):
            return coarse[(k + shift) % coarse_layers]

        return [each(lambda a, b: jnp.where(even, a, b), layer(k), layer(k + half)) for k in range(half)]

    def shifted(plane):
        return {n: each(lambda v: turned(v, n, 1), plane) for n in (1, 2, 3, -1, -2, -3)} | {0: plane}

    def mixed_lanes(t, even_by, odd_by):
        trio = [
            t[even_by + n]
            if even_by == odd_by
            else each(lambda a, b: jnp.where(even, a, b), t[even_by + n], t[odd_by + n])
            for n in (2, 0, -2)
        ]
        return trio[1], row_filtered(each(lambda *v: blend(*v, coarse_along_y), *trio), coarse_along_x)

    def advance_packed(coarse, pulls, keeps):
        turns = [shifted(c) for c in coarse]
        planes = [mixed_lanes(t, 0, 0)[1] for t in turns]
        low, high = mixed_lanes(turns[-1], -1, 1)[1], mixed_lanes(turns[0], -1, 1)[1]
        ring = [low] + planes + [high]
        return [
            stepped(ring[k : k + 3], coarse[k], pulls[k], keeps[k], coarse_along_z) for k in range(half)
        ]

    def advance_opened(coarse, pulls, keeps):
        turns = [shifted(c) for c in coarse]

        def opened(k):
            k = k % coarse_layers
            return mixed_lanes(turns[k % half], *((0, 1) if k < half else (-1, 0)))

        ring = [opened(k) for k in range(-1, coarse_depth + 1)]
        return [
            stepped([r[1] for r in ring[k : k + 3]], ring[k + 1][0], pulls[k], keeps[k], coarse_along_z)
            for k in range(coarse_depth)
        ]

    def open_lanes(coarse, k):
        both = coarse[k % half]
        if k < half:
            return each(lambda v: jnp.where(even, v, turned(v, 1, 1)), both)
        return each(lambda v: jnp.where(even, turned(v, -1, 1), v), both)

    def plus(first, second):
        return [
            b if a is None else a if b is None else each(jnp.add, a, b) for a, b in zip(first, second)
        ]

    def packed_in(ref, *where):
        return [plane_of(ref, *where, k) for k in range(half)]

    def grown(ks):
        return sorted({(k + n) % layers for k in ks for n in (-1, 0, 1)})

    def origin(s, k):
        return raw_plane(state, s, k)

    def held_plane(s, turn, k, first):
        return first(s, k) if turn == 0 else plane_of(field, s, k)

    def spread(s, turn, ks, first=origin):
        for k in ks:
            sides = each(lambda v: lane_filtered(v, 1, fine_along_y), held_plane(s, turn, k, first))
            put(mixed, row_filtered(sides, fine_along_x), turn % 2, s, k)

    def settle(s, turn, live, ks, first=origin):
        for k in ks:
            trio = [
                plane_of(mixed, turn % 2, s, n % layers) if n % layers in live else None
                for n in (k - 1, k, k + 1)
            ]
            held = held_plane(s, turn, k, first) if k in live else None
            put(field, stepped(trio, held, plane_of(pull, k), plane_of(keep, k), fine_along_z), s, k)

    own_layers, own_coarse = list(range(depth)), list(range(coarse_depth))
    all_layers, all_coarse = list(range(layers)), list(range(coarse_layers))
    nothing = (jnp.zeros((SUBLANES, lanes), jnp.float32),) * coarse_vectors

    def each_fine(coarse, k):
        return tuple(coarse[k // 2][j // 2] for j in range(vectors))

    def sent_on(s, guess, ks):
        for k in ks:
            if guess[k // 2] is not None:
                put(field, each(jnp.subtract, plane_of(field, s, k), each_fine(guess, k)), s, k)

    def hand_in(ref, plane, k):
        for stride, vector in zip(strides, plane):
            ref[0, k, stride, :] = vector

    @pl.when(leads)
    def _():
        for j in range(2, groups):
            @pl.when(group - j >= 0)
            def _():
                signal(far_open, leader(group - j, 0))

        rate_load.wait()
        for i in others:
            rate_copy(i).start()
        state_load.wait()

        @pl.when(last)
        def _():
            for q in range(parts):
                round_copy(offset_to(q)).start()

        prepare(own_layers)
        lives = [own_layers]
        for _ in range(FINE):
            lives.append(grown(lives[-1]))
        ready_now = [own_layers]
        for turn in range(FINE):
            known = set(ready_now[-1])
            ready_now.append([
                k for k in own_layers
                if all(n % layers in known or n % layers not in lives[turn] for n in (k - 1, k, k + 1))
            ])

        def early(s):
            for turn in range(FINE):
                spread(s, turn, ready_now[turn])
                settle(s, turn, lives[turn], ready_now[turn + 1])

        def late(turn):
            for s in (0, 1):
                spread(s, turn, [k for k in lives[turn] if k not in ready_now[turn]])
            for s in (0, 1):
                settle(
                    s, turn, lives[turn], [k for k in lives[turn + 1] if k not in ready_now[turn + 1]]
                )

        def begin_of(s):
            begin = [raw_restricted(state, k, s) for k in own_coarse]
            begin += [None] * (coarse_layers - coarse_depth)
            return begin, all_filtered(begin)

        early(1)
        begins = {1: begin_of(1)}
        own_pulls, own_keeps = coarse_rates(own_coarse)
        pl.semaphore_wait(here, 1)

        @pl.when(group > 0)
        def _():
            signal(near_open, leader(group - 1, 0))

        raw_copy().wait_recv()
        early(0)
        begins[0] = begin_of(0)
        drain(arrive.at[1], rates.at[pl.ds(0, depth * (parts - 1))])
        for i in others:
            hand_copy(i).start()

        @pl.when(~last)
        def _():
            pl.semaphore_wait(near_open, 1)
            next_copy().start()

        prepare([k for k in all_layers if k not in own_layers])
        for turn in range(FINE):
            late(turn)
        live = lives[-1]
        pulls, keeps = coarse_rates(all_coarse[coarse_depth:])
        pulls, keeps = own_pulls | pulls, own_keeps | keeps
        guesses = []
        for s, gate in ((0, jnp.where(group > 0, 1.0, 0.0)), (1, None)):
            guess = advance(*begins[s], pulls, keeps, all_coarse)
            if gate is not None:
                guess = [g if g is None else each(lambda v: gate * v, g) for g in guess]
            guesses.append(guess)
        for s in (0, 1):
            for k in all_layers:
                if k not in live:
                    put(field, (jnp.zeros((SUBLANES, lanes), jnp.float32),) * vectors, s, k)

        def fine_of(s, k):
            return plane_of(field, s, 2 * k), plane_of(field, s, 2 * k + 1)

        def zero_guess(s, k):
            return guesses[s][k] if guesses[s][k] is not None else nothing

        both = [
            restricted_and_filtered(*fine_of(0, k), guesses[0][k])
            if 2 * k in live
            else (each(jnp.negative, zero_guess(0, k)), coarse_filtered(each(jnp.negative, zero_guess(0, k))))
            for k in all_coarse
        ]
        term = [b[0] for b in both]
        after = [
            each(jnp.subtract, restricted(*fine_of(1, k)) if 2 * k in live else nothing, zero_guess(1, k))
            for k in all_coarse
        ]
        run = plus(advance(term, [b[1] for b in both], pulls, keeps, all_coarse), after)
        for i in range(parts):
            shift = i * coarse_depth
            for k, c in enumerate(packed(run, shift)):
                put(shares, c, i, 0, k)
            for k in own_coarse:
                put(crown, run[(k + shift) % coarse_layers], i, k)

        @pl.when(last)
        def _():
            for q in range(parts):
                crown_copy(offset_to(q)).start()

        @pl.when(~last & (group > 0))
        def _():
            for q in range(parts):
                wrap_copy(offset_to(q)).start()

        for i in others:
            share_copy(i, 0).start()
        for i in range(parts):
            for k, c in enumerate(packed(term, i * coarse_depth)):
                put(shares, c, i, 1, k)
        sent_on(1, guesses[1], all_layers)

        @pl.when(group == 0)
        def _():
            for i in others:
                part_copy(i).start()
                share_copy(i, 1).start()

        @pl.when(group + 2 < groups)
        def _():
            pl.semaphore_wait(far_open, groups - 2 - group)

        drain(arrive.at[3], shares_in.at[0])
        total = packed_in(shares, 0, 0)
        for r in others:
            total = plus(total, packed_in(shares_in, 0, r - 1))
        for k in range(half):
            put(sums, total[k], group, k)
        for j in reversed(range(1, groups)):
            @pl.when(group + j < groups)
            def _():
                sum_copy(j).start()

        @pl.when(direct)
        def _():
            first_copy().start()

        @pl.when(group > 0)
        def _():
            for i in others:
                share_copy(i, 1).start()

        packed_pulls, packed_keeps = packed(pulls), packed(keeps)

        def twice(coarse):
            for _ in range(2):
                coarse = advance_packed(coarse, packed_pulls, packed_keeps)
            return coarse

        @pl.when(group > 0)
        def _():
            drain(arrive.at[line], sums.at[0])
            for i in others:
                part_copy(i).start()

        @pl.when(group == 0)
        def _():
            for k in range(half):
                put(base, nothing, k)

        @pl.when(group > 0)
        def _():
            def pass_group(index, coarse):
                coarse = twice(coarse)
                drain(arrive.at[line + index], sums.at[index])
                return plus(coarse, packed_in(sums, index))

            coarse = lax.fori_loop(1, group, pass_group, packed_in(sums, 0))
            for k in range(half):
                put(base, coarse[k], k)

        coarse = packed_in(base)
        ahead = advance_opened(coarse, pulls, keeps)

        @pl.when(group > 0)
        def _():
            for k in own_coarse:
                put(heads, open_lanes(coarse, k), 0, k)
                put(heads, ahead[k], 1, k)
            head_copy().start()

        drain(arrive.at[6], shares_in.at[1])
        middle = packed_in(shares, 0, 1)
        for r in others:
            middle = plus(middle, packed_in(shares_in, 1, r - 1))
        finish = advance_opened(
            plus(advance_packed(coarse, packed_pulls, packed_keeps), middle), pulls, keeps
        )
        corr_copy().wait_recv()
        drain(arrive.at[4], parts_in)
        for k in own_layers:
            hand_in(next_ref, each(jnp.add, plane_of(corr_in, k), each_fine(ahead, k)), k)
            held = plane_of(field, 1, k)
            for r in others:
                held = each(jnp.add, held, plane_of(parts_in, r - 1, k))
            hand_in(end_ref, each(jnp.add, held, each_fine(finish, k)), k)
        away = pl.ds(0, depth * (parts - 1))
        drain(leave.at[0], rates.at[away])
        drain(leave.at[1], rates.at[away])
        @pl.when(~last)
        def _():
            drain(leave.at[2], raw_in.at[own])

        drain(leave.at[4], shares_in.at[0])
        drain(leave.at[8], shares_in.at[1])
        drain(leave.at[5], parts_in)
        for j in range(1, groups):
            @pl.when(groups - 1 - group == j)
            def _():
                drain(leave.at[7], sums.at[pl.ds(0, j)])

        @pl.when(last)
        def _():
            drain(leave.at[2], raw_in)
            drain(leave.at[3], crown_in)

        @pl.when(~last & (group > 0))
        def _():
            drain(leave.at[3], wraps.at[0])

        @pl.when(direct)
        def _():
            drain(leave.at[3], sums.at[0])

        @pl.when(proxy)
        def _():
            drain(arrive.at[7], raw_in)
            forward_copy().start()

            def pass_group(index, coarse):
                coarse = twice(coarse)
                drain(arrive.at[line + index], wraps.at[index])
                for r in range(parts):
                    coarse = plus(coarse, packed_in(wraps, index, r))
                return coarse

            coarse = lax.fori_loop(1, groups - 1, pass_group, packed_in(sums, 0))
            coarse = advance_packed(coarse, packed_pulls, packed_keeps)
            coarse = advance_opened(coarse, pulls, keeps)
            drain(arrive.at[line + groups - 1], crown_in)
            for k in own_coarse:
                following = coarse[k]
                for r in range(parts):
                    following = each(jnp.add, following, plane_of(crown_in, r, k))
                put(heads, following, 0, k)
                put(heads, nothing, 1, k)
            head_copy().start()
            drain(leave.at[3], raw_in)

        @pl.when(~direct)
        def _():
            drain(leave.at[6], heads)

    @pl.when(helps)
    def _():
        signal(here, leader(group, 0))
        state_load.wait()
        raw_copy().start()
        rate_load.wait()
        prepare(own_layers)
        raw_copy().wait_send()
        for i in others:
            side_copy(i).start()
        away = pl.ds(0, depth * (parts - 1))
        drain(arrive.at[2], rates.at[away])
        drain(arrive.at[1], rates.at[away])
        prepare([k for k in all_layers if k not in own_layers])
        pulls, keeps = coarse_rates(all_coarse)

        def solve(s, gate):
            def first(s, k):
                return raw_plane(state, 0, k) if s == 0 else raw_plane(raw_in, k)

            begin = [restricted(first(s, 2 * k), first(s, 2 * k + 1)) for k in all_coarse]
            guess = advance(begin, all_filtered(begin), pulls, keeps, own_coarse)
            if gate is not None:
                guess = [g if g is None else each(lambda v: gate * v, g) for g in guess]
            wanted = [own_layers]
            for _ in range(1, FINE):
                wanted.append(grown(wanted[-1]))
            for turn in range(FINE):
                reach = wanted[FINE - 1 - turn]
                spread(s, turn, grown(reach), first)
                settle(s, turn, all_layers, reach, first)
            sent_on(s, guess, own_layers)

        solve(0, jnp.where(group > 0, 1.0, 0.0))
        corr_copy().start()
        packed_pulls, packed_keeps = packed(pulls), packed(keeps)

        def arrived(index):
            drain(arrive.at[line + index], wraps.at[index])

        def with_arrived(coarse, index):
            for r in range(parts):
                coarse = plus(coarse, packed_in(wraps, index, r))
            return coarse

        def twice(coarse):
            for _ in range(2):
                coarse = advance_packed(coarse, packed_pulls, packed_keeps)
            return coarse

        def second_solve():
            solve(1, None)
            before = [field_restricted(1, k) for k in own_coarse]
            sent_on(1, before, own_layers)

        @pl.when(direct)
        def _():
            for k in own_layers:
                hand_in(end_ref, plane_of(field, 0, k), k)
            drain(arrive.at[line], wraps.at[0, 0])
            coarse = packed_in(wraps, 0, 0)
            if groups > 2:
                coarse = twice(coarse)
            drain(arrive.at[7], raw_in)
            second_solve()
            drain(leave.at[2], corr_in)
            drain(leave.at[1], rates.at[away])
            for index in range(1, groups - 1):
                arrived(index)
                coarse = with_arrived(coarse, index)
                if index < groups - 2:
                    coarse = twice(coarse)
            coarse = advance_packed(coarse, packed_pulls, packed_keeps)
            coarse = advance_opened(coarse, pulls, keeps)
            for k in own_layers:
                put(field, each(jnp.add, plane_of(field, 1, k), each_fine(coarse, k)), 1, k)
            drain(arrive.at[line + groups - 1], crown_in)
            for k in own_layers:
                following = plane_of(field, 1, k)
                for r in range(parts):
                    offset = each_fine([plane_of(crown_in, r, c) for c in own_coarse], k)
                    following = each(jnp.add, following, offset)
                hand_in(next_ref, following, k)

        @pl.when(proxy)
        def _():
            drain(arrive.at[7], raw_in)

        @pl.when(group > 0)
        def _():
            drain(arrive.at[7], raw_in.at[own])
            for i in others:
                across_copy(i).start()
            drain(arrive.at[0], raw_in.at[away])

        @pl.when(~direct)
        def _():
            second_solve()
            drain(leave.at[2], corr_in)
            drain(leave.at[1], rates.at[away])

            @pl.when(group > 0)
            def _():
                drain(leave.at[3], raw_in.at[away])

            head_copy().wait_recv()
            for k in own_layers:
                coarse, ahead = ([plane_of(heads_in, n, c) for c in own_coarse] for n in range(2))
                hand_in(next_ref, each(jnp.add, plane_of(field, 1, k), each_fine(coarse, k)), k)
                hand_in(end_ref, each(jnp.add, plane_of(field, 0, k), each_fine(ahead, k)), k)


def hand_out_kernel(end_ref, next_ref, end_out, next_out, sems):
    copies = [
        pltpu.make_async_copy(end_ref, end_out, sems.at[0]),
        pltpu.make_async_copy(next_ref, next_out, sems.at[1]),
    ]
    for copy in copies:
        copy.start()
    for copy in copies:
        copy.wait()


def hand_out(end, following):
    return pl.pallas_call(
        hand_out_kernel,
        out_shape=[jax.ShapeDtypeStruct(end.shape, end.dtype)] * 2,
        in_specs=[pl.BlockSpec(memory_space=pltpu.VMEM)] * 2,
        out_specs=[pl.BlockSpec(memory_space=pl.ANY)] * 2,
        scratch_shapes=[pltpu.SemaphoreType.DMA((2,))],
    )(*(pltpu.with_memory_space_constraint(x, pltpu.VMEM) for x in (end, following)))


def solution(mesh):
    slabs, parts = mesh.shape["tm"], mesh.shape["gz"]

    def per_device(starts, cell_rates):
        depth, rows, lanes = cell_rates.shape
        layers = depth * parts
        groups = slabs // 2
        vectors = rows // SUBLANES
        fine = (vectors, SUBLANES, lanes)
        coarse = (vectors // 2, SUBLANES, lanes)
        packed = (layers // 4, *coarse)
        lead = (depth // 2, *coarse)
        aside = max(parts - 1, 1)
        dma = pltpu.SemaphoreType.DMA

        def vmem(*shape):
            return pltpu.VMEM(shape, jnp.float32)

        ends = pl.pallas_call(
            functools.partial(kernel, slabs, parts),
            out_shape=[pltpu.VMEM(starts.shape, jnp.float32)] * 2,
            in_specs=[pl.BlockSpec(memory_space=pl.ANY)] * 2,
            out_specs=[pl.BlockSpec(memory_space=pltpu.VMEM)] * 2,
            scratch_shapes=[
                vmem(2, layers, rows, lanes),
                vmem(layers, rows, lanes),
                vmem(layers, *fine),
                vmem(layers, *fine),
                vmem(2, 2, layers, *fine),
                vmem(2, layers, *fine),
                vmem(parts, 2, *packed),
                vmem(2, aside, *packed),
                vmem(groups, *packed),
                vmem(groups, parts, *packed),
                vmem(parts, *lead),
                vmem(parts, *lead),
                vmem(2, *lead),
                vmem(2, *lead),
                vmem(depth, *fine),
                vmem(aside, depth, *fine),
                vmem(*packed),
                vmem(layers, rows, lanes),
                pltpu.SemaphoreType.REGULAR((3,)),
                dma((9,)),
                dma((8 + groups,)),
            ],
            compiler_params=pltpu.CompilerParams(collective_id=0, has_side_effects=True),
        )(starts, cell_rates)
        return hand_out(*ends)

    return jax.shard_map(
        per_device,
        mesh=mesh,
        in_specs=(P("tm", "gz", None, None), P("gz", None, None)),
        out_specs=(P("tm", "gz", None, None), P("tm", "gz", None, None)),
        check_vma=False,
    )
```

```python
import functools

import jax
import jax.numpy as jnp
from jax import lax
from jax.experimental import pallas as pl
from jax.experimental.pallas import tpu as pltpu
from jax.sharding import PartitionSpec as P

MESH = pl.DeviceIdType.MESH
FINE = 4
SUBLANES = 8

fine_along_z = (0.1, 0.12)
fine_along_x = (0.15, 0.12)
fine_along_y = (0.2, 0.12)
coarse_along_z = (0.2, 0.25)
coarse_along_x = (0.3, 0.25)
coarse_along_y = (0.4, 0.25)


def blend(behind, middle, beyond, along):
    courant, diffuse = along
    center = 1.0 - 2.0 * diffuse
    before, after = (diffuse + 0.5 * courant) / center, (diffuse - 0.5 * courant) / center
    if middle is None:
        return before * behind if beyond is None else after * beyond
    if behind is None:
        return middle if beyond is None else middle + after * beyond
    if beyond is None:
        return middle + before * behind
    return middle + (before * behind + after * beyond)


def centers(*alongs):
    product = 1.0
    for _, diffuse in alongs:
        product *= 1.0 - 2.0 * diffuse
    return product


def turned(values, by, dim):
    return pltpu.roll(values, by % values.shape[dim], dim)


def lane_filtered(values, by, along):
    return blend(turned(values, by, 1), values, turned(values, -by, 1), along)


def row_filtered(plane, along):
    ring = (turned(plane[-1], 1, 0), *plane, turned(plane[0], -1, 0))
    return tuple(blend(*ring[j : j + 3], along) for j in range(len(plane)))


def each(f, *planes):
    return tuple(f(*vectors) for vectors in zip(*planes))


def kernel(
    slabs, parts, starts_ref, rates_ref, end_ref, next_ref,
    state, rates, pull, keep, mixed, field, shares, shares_in, sums, wraps, crown, crown_in,
    heads, heads_in, corr_in, parts_in, base, raw_in,
    ready, leave, arrive,
):
    depth, rows, lanes = rates_ref.shape
    layers = depth * parts
    groups = slabs // 2
    coarse_layers, coarse_rows, coarse_depth = layers // 2, rows // 2, depth // 2
    half = coarse_layers // 2
    vectors = rows // SUBLANES
    coarse_vectors = vectors // 2
    me, part = lax.axis_index("tm"), lax.axis_index("gz")
    group, place = me // 2, lax.rem(me, 2)
    leads, helps = place == 1, place == 0
    last = group == groups - 1
    direct, proxy = (group == 0) & (part == 0), (group == 0) & (part > 0)

    def block(r):
        return pl.ds(r % parts * depth, depth)

    own = block(0)
    rate_load = pltpu.make_async_copy(rates_ref, rates.at[own], leave.at[5])
    state_load = pltpu.make_async_copy(starts_ref.at[0], state.at[place, own], leave.at[6])
    def leader(g, i):
        return {"tm": 2 * g + 1, "gz": lax.rem(part + i, parts)}

    def helper(g, i):
        return {"tm": 2 * g, "gz": lax.rem(part + i, parts)}

    def signal(sem, peer):
        pl.semaphore_signal(sem, inc=1, device_id=peer, device_id_type=MESH)

    def remote(src, dst, send_sem, recv_sem, peer):
        return pltpu.make_async_remote_copy(
            src_ref=src, dst_ref=dst, send_sem=send_sem, recv_sem=recv_sem,
            device_id=peer, device_id_type=MESH,
        )

    others = range(1, parts)
    barrier = pltpu.get_barrier_semaphore()
    here, near_open, far_open = (ready.at[n] for n in range(3))
    line = 8

    @pl.when(leads)
    def _():
        for i in others:
            signal(barrier, leader(group, i))
        rate_load.start()
        state_load.start()
        signal(barrier, helper(group, 0))
        for j in range(1, groups):
            @pl.when(group + j < groups)
            def _():
                signal(barrier, leader(group + j, 0))

        @pl.when(proxy)
        def _():
            for j in range(1, groups):
                for i in others:
                    signal(barrier, leader(j, i))

    @pl.when(helps)
    def _():
        state_load.start()
        rate_load.start()
        for i in others:
            signal(barrier, helper(group, i))

        @pl.when(direct)
        def _():
            for j in range(1, groups):
                for i in range(parts):
                    signal(barrier, leader(j, i))

    earlier = group + jnp.where(group > 0, parts - jnp.where(part > 0, 1, 0), 0)
    pl.semaphore_wait(barrier, jnp.where(leads, parts - 1 + earlier, parts))

    def drain(sem, ref):
        pltpu.make_async_copy(ref, ref, sem).wait()

    def raw_copy():
        piece = state.at[0, own]
        return remote(piece, piece, leave.at[0], arrive.at[0], leader(group, 0))

    def rate_copy(i):
        return remote(
            rates.at[own], rates.at[block(parts - i)],
            leave.at[0], arrive.at[1], leader(group, i),
        )

    def hand_copy(i):
        piece = rates.at[block(i)]
        return remote(piece, piece, leave.at[1], arrive.at[1], helper(group, 0))

    def side_copy(i):
        return remote(
            state.at[0, own], state.at[0, block(parts - i)], leave.at[1], arrive.at[2], helper(group, i)
        )

    def offset_to(q):
        return lax.rem(q + parts - part, parts)

    def home(i):
        q = lax.rem(part + i, parts)
        return {"tm": jnp.where(q == 0, 0, 1), "gz": q}

    def raw_next(i, send_sem, peer):
        r = lax.rem(parts - i, parts)
        return remote(state.at[1, own], raw_in.at[pl.ds(r * depth, depth)], send_sem, arrive.at[7], peer)

    def next_copy():
        return raw_next(0, leave.at[2], helper(group + 1, 0))

    def across_copy(i):
        return remote(raw_in.at[own], raw_in.at[block(parts - i)], leave.at[3], arrive.at[0], helper(group, i))

    def round_copy(i):
        return raw_next(i, leave.at[2], home(i))

    def forward_copy():
        return remote(raw_in, raw_in, leave.at[3], arrive.at[7], helper(0, 0))

    def wrap_copy(i):
        return remote(
            shares.at[i, 0], wraps.at[group, lax.rem(parts - i, parts)], leave.at[3], arrive.at[line + group],
            home(i),
        )

    def first_copy():
        return remote(sums.at[0], wraps.at[0, 0], leave.at[3], arrive.at[line], helper(0, 0))

    def crown_copy(i):
        return remote(
            crown.at[i], crown_in.at[lax.rem(parts - i, parts)], leave.at[3], arrive.at[line + group],
            home(i),
        )

    def share_copy(i, n):
        return remote(
            shares.at[i, n], shares_in.at[n, parts - i - 1], leave.at[4 if n == 0 else 8],
            arrive.at[3 if n == 0 else 6], leader(group, i),
        )

    def sum_copy(j):
        piece = sums.at[group]
        return remote(piece, piece, leave.at[7], arrive.at[line + group], leader(group + j, 0))

    def part_copy(i):
        return remote(
            field.at[1, block(i)], parts_in.at[parts - i - 1], leave.at[5], arrive.at[4], leader(group, i)
        )

    def corr_copy():
        return remote(field.at[0, own], corr_in, leave.at[2], arrive.at[5], leader(group, 0))

    def head_copy():
        return remote(heads, heads_in, leave.at[6], arrive.at[3], helper(group, 0))

    even = lax.rem(lax.broadcasted_iota(jnp.int32, (SUBLANES, lanes), 1), 2) == 0
    fine_center = centers(fine_along_y, fine_along_x, fine_along_z)
    coarse_center = centers(coarse_along_y, coarse_along_x, coarse_along_z)
    strides = [pl.ds(j, SUBLANES, stride=vectors) for j in range(vectors)]

    def raw_plane(ref, *where):
        return tuple(ref[(*where, stride)] for stride in strides)

    def plane_of(ref, *where):
        return tuple(ref[(*where, j)] for j in range(ref.shape[-3]))

    def put(ref, plane, *where):
        for j, vector in enumerate(plane):
            ref[(*where, j)] = vector

    def prepare(ks):
        for k in ks:
            rate = raw_plane(rates, k)
            put(pull, each(lambda r: r * fine_center, rate), k)
            put(keep, each(lambda r: 1.0 - r, rate), k)

    def restricted(upper, lower):
        merged = each(jnp.add, upper, lower)
        averages = []
        for j in range(coarse_vectors):
            total = merged[2 * j] + merged[2 * j + 1]
            pair_sum = total + jnp.where(even, turned(total, -1, 1), turned(total, 1, 1))
            averages.append(pair_sum * 0.125)
        return tuple(averages)

    def restricted_and_filtered(upper, lower, guess):
        merged = each(jnp.add, upper, lower)
        total = tuple(merged[2 * j] + merged[2 * j + 1] for j in range(coarse_vectors))
        if guess is not None:
            total = each(lambda t, g: t - 4.0 * g, total, guess)
        total = each(lambda t: t * 0.125, total)
        t = shifted(total)

        def pair(n):
            return each(lambda here, a, b: here + jnp.where(even, a, b), t[n], t[n - 1], t[n + 1])

        here = pair(0)
        sides = each(lambda *v: blend(*v, coarse_along_y), pair(2), here, pair(-2))
        return here, row_filtered(sides, coarse_along_x)

    def raw_restricted(ref, k, *lead):
        return restricted(raw_plane(ref, *lead, 2 * k), raw_plane(ref, *lead, 2 * k + 1))

    def field_restricted(s, k):
        return restricted(plane_of(field, s, 2 * k), plane_of(field, s, 2 * k + 1))

    def coarse_rates(ks):
        weights = {k: raw_restricted(rates, k) for k in ks}
        return (
            {k: each(lambda v: v * coarse_center, w) for k, w in weights.items()},
            {k: each(lambda v: 1.0 - v, w) for k, w in weights.items()},
        )

    def stepped(trio, held, pulls, keeps, along):
        behind, middle, beyond = trio
        if middle is None and behind is not None and beyond is not None:
            deep = each(
                lambda b, f: blend(b, None, None, along) + blend(None, None, f, along), behind, beyond
            )
        else:
            there = [p for p in trio if p is not None]

            def mix(*given):
                given = iter(given)
                return blend(*(None if p is None else next(given) for p in trio), along)

            deep = each(mix, *there)
        if held is None:
            return each(jnp.multiply, pulls, deep)
        return each(lambda p, d, q, h: p * d + q * h, pulls, deep, keeps, held)

    def coarse_filtered(plane):
        return row_filtered(each(lambda v: lane_filtered(v, 2, coarse_along_y), plane), coarse_along_x)

    def advance(coarse, mixes, pulls, keeps, wanted):
        moved = [None] * coarse_layers
        for k in wanted:
            trio = mixes[k - 1], mixes[k], mixes[(k + 1) % coarse_layers]
            if any(p is not None for p in trio):
                moved[k] = stepped(trio, coarse[k], pulls[k], keeps[k], coarse_along_z)
        return moved

    def all_filtered(coarse):
        return [None if c is None else coarse_filtered(c) for c in coarse]

    def packed(coarse, shift=0):
        def layer(k):
            return coarse[(k + shift) % coarse_layers]

        return [each(lambda a, b: jnp.where(even, a, b), layer(k), layer(k + half)) for k in range(half)]

    def shifted(plane):
        return {n: each(lambda v: turned(v, n, 1), plane) for n in (1, 2, 3, -1, -2, -3)} | {0: plane}

    def mixed_lanes(t, even_by, odd_by):
        trio = [
            t[even_by + n]
            if even_by == odd_by
            else each(lambda a, b: jnp.where(even, a, b), t[even_by + n], t[odd_by + n])
            for n in (2, 0, -2)
        ]
        return trio[1], row_filtered(each(lambda *v: blend(*v, coarse_along_y), *trio), coarse_along_x)

    def advance_packed(coarse, pulls, keeps):
        turns = [shifted(c) for c in coarse]
        planes = [mixed_lanes(t, 0, 0)[1] for t in turns]
        low, high = mixed_lanes(turns[-1], -1, 1)[1], mixed_lanes(turns[0], -1, 1)[1]
        ring = [low] + planes + [high]
        return [
            stepped(ring[k : k + 3], coarse[k], pulls[k], keeps[k], coarse_along_z) for k in range(half)
        ]

    def advance_opened(coarse, pulls, keeps):
        turns = [shifted(c) for c in coarse]

        def opened(k):
            k = k % coarse_layers
            return mixed_lanes(turns[k % half], *((0, 1) if k < half else (-1, 0)))

        ring = [opened(k) for k in range(-1, coarse_depth + 1)]
        return [
            stepped([r[1] for r in ring[k : k + 3]], ring[k + 1][0], pulls[k], keeps[k], coarse_along_z)
            for k in range(coarse_depth)
        ]

    def open_lanes(coarse, k):
        both = coarse[k % half]
        if k < half:
            return each(lambda v: jnp.where(even, v, turned(v, 1, 1)), both)
        return each(lambda v: jnp.where(even, turned(v, -1, 1), v), both)

    def plus(first, second):
        return [
            b if a is None else a if b is None else each(jnp.add, a, b) for a, b in zip(first, second)
        ]

    def packed_in(ref, *where):
        return [plane_of(ref, *where, k) for k in range(half)]

    def grown(ks):
        return sorted({(k + n) % layers for k in ks for n in (-1, 0, 1)})

    def origin(s, k):
        return raw_plane(state, s, k)

    def held_plane(s, turn, k, first):
        return first(s, k) if turn == 0 else plane_of(field, s, k)

    def spread(s, turn, ks, first=origin):
        for k in ks:
            sides = each(lambda v: lane_filtered(v, 1, fine_along_y), held_plane(s, turn, k, first))
            put(mixed, row_filtered(sides, fine_along_x), turn % 2, s, k)

    def settle(s, turn, live, ks, first=origin):
        for k in ks:
            trio = [
                plane_of(mixed, turn % 2, s, n % layers) if n % layers in live else None
                for n in (k - 1, k, k + 1)
            ]
            held = held_plane(s, turn, k, first) if k in live else None
            put(field, stepped(trio, held, plane_of(pull, k), plane_of(keep, k), fine_along_z), s, k)

    own_layers, own_coarse = list(range(depth)), list(range(coarse_depth))
    all_layers, all_coarse = list(range(layers)), list(range(coarse_layers))
    nothing = (jnp.zeros((SUBLANES, lanes), jnp.float32),) * coarse_vectors

    def each_fine(coarse, k):
        return tuple(coarse[k // 2][j // 2] for j in range(vectors))

    def sent_on(s, guess, ks):
        for k in ks:
            if guess[k // 2] is not None:
                put(field, each(jnp.subtract, plane_of(field, s, k), each_fine(guess, k)), s, k)

    def hand_in(ref, plane, k):
        for stride, vector in zip(strides, plane):
            ref[0, k, stride, :] = vector

    @pl.when(leads)
    def _():
        for j in range(2, groups):
            @pl.when(group - j >= 0)
            def _():
                signal(far_open, leader(group - j, 0))

        rate_load.wait()
        for i in others:
            rate_copy(i).start()
        state_load.wait()

        @pl.when(last)
        def _():
            for q in range(parts):
                round_copy(offset_to(q)).start()

        prepare(own_layers)
        lives = [own_layers]
        for _ in range(FINE):
            lives.append(grown(lives[-1]))
        ready_now = [own_layers]
        for turn in range(FINE):
            known = set(ready_now[-1])
            ready_now.append([
                k for k in own_layers
                if all(n % layers in known or n % layers not in lives[turn] for n in (k - 1, k, k + 1))
            ])

        def early(s):
            for turn in range(FINE):
                spread(s, turn, ready_now[turn])
                settle(s, turn, lives[turn], ready_now[turn + 1])

        def late(turn):
            for s in (0, 1):
                spread(s, turn, [k for k in lives[turn] if k not in ready_now[turn]])
            for s in (0, 1):
                settle(
                    s, turn, lives[turn], [k for k in lives[turn + 1] if k not in ready_now[turn + 1]]
                )

        def begin_of(s):
            begin = [raw_restricted(state, k, s) for k in own_coarse]
            begin += [None] * (coarse_layers - coarse_depth)
            return begin, all_filtered(begin)

        early(1)
        begins = {1: begin_of(1)}
        own_pulls, own_keeps = coarse_rates(own_coarse)
        pl.semaphore_wait(here, 1)

        @pl.when(group > 0)
        def _():
            signal(near_open, leader(group - 1, 0))

        raw_copy().wait_recv()
        early(0)
        begins[0] = begin_of(0)
        drain(arrive.at[1], rates.at[pl.ds(0, depth * (parts - 1))])
        for i in others:
            hand_copy(i).start()

        @pl.when(~last)
        def _():
            pl.semaphore_wait(near_open, 1)
            next_copy().start()

        prepare([k for k in all_layers if k not in own_layers])
        for turn in range(FINE):
            late(turn)
        live = lives[-1]
        pulls, keeps = coarse_rates(all_coarse[coarse_depth:])
        pulls, keeps = own_pulls | pulls, own_keeps | keeps
        guesses = []
        for s, gate in ((0, jnp.where(group > 0, 1.0, 0.0)), (1, None)):
            guess = advance(*begins[s], pulls, keeps, all_coarse)
            if gate is not None:
                guess = [g if g is None else each(lambda v: gate * v, g) for g in guess]
            guesses.append(guess)
        for s in (0, 1):
            for k in all_layers:
                if k not in live:
                    put(field, (jnp.zeros((SUBLANES, lanes), jnp.float32),) * vectors, s, k)

        def fine_of(s, k):
            return plane_of(field, s, 2 * k), plane_of(field, s, 2 * k + 1)

        def zero_guess(s, k):
            return guesses[s][k] if guesses[s][k] is not None else nothing

        both = [
            restricted_and_filtered(*fine_of(0, k), guesses[0][k])
            if 2 * k in live
            else (each(jnp.negative, zero_guess(0, k)), coarse_filtered(each(jnp.negative, zero_guess(0, k))))
            for k in all_coarse
        ]
        term = [b[0] for b in both]
        after = [
            each(jnp.subtract, restricted(*fine_of(1, k)) if 2 * k in live else nothing, zero_guess(1, k))
            for k in all_coarse
        ]
        run = plus(advance(term, [b[1] for b in both], pulls, keeps, all_coarse), after)
        for i in range(parts):
            shift = i * coarse_depth
            for k, c in enumerate(packed(run, shift)):
                put(shares, c, i, 0, k)
            for k in own_coarse:
                put(crown, run[(k + shift) % coarse_layers], i, k)

        @pl.when(last)
        def _():
            for q in range(parts):
                crown_copy(offset_to(q)).start()

        @pl.when(~last & (group > 0))
        def _():
            for q in range(parts):
                wrap_copy(offset_to(q)).start()

        @pl.when(~last)
        def _():
            for i in others:
                share_copy(i, 0).start()

        for i in range(parts):
            for k, c in enumerate(packed(term, i * coarse_depth)):
                put(shares, c, i, 1, k)
        sent_on(1, guesses[1], all_layers)

        @pl.when(group == 0)
        def _():
            for i in others:
                part_copy(i).start()
                share_copy(i, 1).start()

        @pl.when(group + 2 < groups)
        def _():
            pl.semaphore_wait(far_open, groups - 2 - group)

        @pl.when(~last)
        def _():
            drain(arrive.at[3], shares_in.at[0])
            total = packed_in(shares, 0, 0)
            for r in others:
                total = plus(total, packed_in(shares_in, 0, r - 1))
            for k in range(half):
                put(sums, total[k], group, k)

        for j in reversed(range(1, groups)):
            @pl.when(group + j < groups)
            def _():
                sum_copy(j).start()

        @pl.when(direct)
        def _():
            first_copy().start()

        @pl.when(group > 0)
        def _():
            for i in others:
                share_copy(i, 1).start()

        packed_pulls, packed_keeps = packed(pulls), packed(keeps)

        def twice(coarse):
            for _ in range(2):
                coarse = advance_packed(coarse, packed_pulls, packed_keeps)
            return coarse

        @pl.when(group > 0)
        def _():
            drain(arrive.at[line], sums.at[0])
            for i in others:
                part_copy(i).start()

        @pl.when(group == 0)
        def _():
            for k in range(half):
                put(base, nothing, k)

        @pl.when(group > 0)
        def _():
            def pass_group(index, coarse):
                coarse = twice(coarse)
                drain(arrive.at[line + index], sums.at[index])
                return plus(coarse, packed_in(sums, index))

            coarse = lax.fori_loop(1, group, pass_group, packed_in(sums, 0))
            for k in range(half):
                put(base, coarse[k], k)

        coarse = packed_in(base)
        ahead = advance_opened(coarse, pulls, keeps)

        @pl.when(group > 0)
        def _():
            for k in own_coarse:
                put(heads, open_lanes(coarse, k), 0, k)
                put(heads, ahead[k], 1, k)
            head_copy().start()

        drain(arrive.at[6], shares_in.at[1])
        middle = packed_in(shares, 0, 1)
        for r in others:
            middle = plus(middle, packed_in(shares_in, 1, r - 1))
        finish = advance_opened(
            plus(advance_packed(coarse, packed_pulls, packed_keeps), middle), pulls, keeps
        )
        corr_copy().wait_recv()
        drain(arrive.at[4], parts_in)
        for k in own_layers:
            hand_in(next_ref, each(jnp.add, plane_of(corr_in, k), each_fine(ahead, k)), k)
            held = plane_of(field, 1, k)
            for r in others:
                held = each(jnp.add, held, plane_of(parts_in, r - 1, k))
            hand_in(end_ref, each(jnp.add, held, each_fine(finish, k)), k)
        away = pl.ds(0, depth * (parts - 1))
        drain(leave.at[0], rates.at[away])
        drain(leave.at[1], rates.at[away])
        @pl.when(~last)
        def _():
            drain(leave.at[2], raw_in.at[own])

        @pl.when(~last)
        def _():
            drain(leave.at[4], shares_in.at[0])

        drain(leave.at[8], shares_in.at[1])
        drain(leave.at[5], parts_in)
        for j in range(1, groups):
            @pl.when(groups - 1 - group == j)
            def _():
                drain(leave.at[7], sums.at[pl.ds(0, j)])

        @pl.when(last)
        def _():
            drain(leave.at[2], raw_in)
            drain(leave.at[3], crown_in)

        @pl.when(~last & (group > 0))
        def _():
            drain(leave.at[3], wraps.at[0])

        @pl.when(direct)
        def _():
            drain(leave.at[3], sums.at[0])

        @pl.when(proxy)
        def _():
            drain(arrive.at[7], raw_in)
            forward_copy().start()

            def pass_group(index, coarse):
                coarse = twice(coarse)
                drain(arrive.at[line + index], wraps.at[index])
                for r in range(parts):
                    coarse = plus(coarse, packed_in(wraps, index, r))
                return coarse

            coarse = lax.fori_loop(1, groups - 1, pass_group, packed_in(sums, 0))
            coarse = advance_packed(coarse, packed_pulls, packed_keeps)
            coarse = advance_opened(coarse, pulls, keeps)
            drain(arrive.at[line + groups - 1], crown_in)
            for k in own_coarse:
                following = coarse[k]
                for r in range(parts):
                    following = each(jnp.add, following, plane_of(crown_in, r, k))
                put(heads, following, 0, k)
                put(heads, nothing, 1, k)
            head_copy().start()
            drain(leave.at[3], raw_in)

        @pl.when(~direct)
        def _():
            drain(leave.at[6], heads)

    @pl.when(helps)
    def _():
        signal(here, leader(group, 0))
        state_load.wait()
        raw_copy().start()
        rate_load.wait()
        prepare(own_layers)
        raw_copy().wait_send()
        for i in others:
            side_copy(i).start()
        away = pl.ds(0, depth * (parts - 1))
        drain(arrive.at[2], rates.at[away])
        drain(arrive.at[1], rates.at[away])
        prepare([k for k in all_layers if k not in own_layers])
        pulls, keeps = coarse_rates(all_coarse)

        def solve(s, gate):
            def first(s, k):
                return raw_plane(state, 0, k) if s == 0 else raw_plane(raw_in, k)

            begin = [restricted(first(s, 2 * k), first(s, 2 * k + 1)) for k in all_coarse]
            guess = advance(begin, all_filtered(begin), pulls, keeps, own_coarse)
            if gate is not None:
                guess = [g if g is None else each(lambda v: gate * v, g) for g in guess]
            wanted = [own_layers]
            for _ in range(1, FINE):
                wanted.append(grown(wanted[-1]))
            for turn in range(FINE):
                reach = wanted[FINE - 1 - turn]
                spread(s, turn, grown(reach), first)
                settle(s, turn, all_layers, reach, first)
            sent_on(s, guess, own_layers)

        solve(0, jnp.where(group > 0, 1.0, 0.0))
        corr_copy().start()
        packed_pulls, packed_keeps = packed(pulls), packed(keeps)

        def arrived(index):
            drain(arrive.at[line + index], wraps.at[index])

        def with_arrived(coarse, index):
            for r in range(parts):
                coarse = plus(coarse, packed_in(wraps, index, r))
            return coarse

        def twice(coarse):
            for _ in range(2):
                coarse = advance_packed(coarse, packed_pulls, packed_keeps)
            return coarse

        def second_solve():
            solve(1, None)
            before = [field_restricted(1, k) for k in own_coarse]
            sent_on(1, before, own_layers)

        @pl.when(direct)
        def _():
            for k in own_layers:
                hand_in(end_ref, plane_of(field, 0, k), k)
            drain(arrive.at[line], wraps.at[0, 0])
            coarse = packed_in(wraps, 0, 0)
            if groups > 2:
                coarse = twice(coarse)
            drain(arrive.at[7], raw_in)
            second_solve()
            drain(leave.at[2], corr_in)
            drain(leave.at[1], rates.at[away])
            for index in range(1, groups - 1):
                arrived(index)
                coarse = with_arrived(coarse, index)
                if index < groups - 2:
                    coarse = twice(coarse)
            coarse = advance_packed(coarse, packed_pulls, packed_keeps)
            coarse = advance_opened(coarse, pulls, keeps)
            for k in own_layers:
                put(field, each(jnp.add, plane_of(field, 1, k), each_fine(coarse, k)), 1, k)
            drain(arrive.at[line + groups - 1], crown_in)
            for k in own_layers:
                following = plane_of(field, 1, k)
                for r in range(parts):
                    offset = each_fine([plane_of(crown_in, r, c) for c in own_coarse], k)
                    following = each(jnp.add, following, offset)
                hand_in(next_ref, following, k)

        @pl.when(proxy)
        def _():
            drain(arrive.at[7], raw_in)

        @pl.when(group > 0)
        def _():
            drain(arrive.at[7], raw_in.at[own])
            for i in others:
                across_copy(i).start()
            drain(arrive.at[0], raw_in.at[away])

        @pl.when(~direct)
        def _():
            second_solve()
            drain(leave.at[2], corr_in)
            drain(leave.at[1], rates.at[away])

            @pl.when(group > 0)
            def _():
                drain(leave.at[3], raw_in.at[away])

            head_copy().wait_recv()
            for k in own_layers:
                coarse, ahead = ([plane_of(heads_in, n, c) for c in own_coarse] for n in range(2))
                hand_in(next_ref, each(jnp.add, plane_of(field, 1, k), each_fine(coarse, k)), k)
                hand_in(end_ref, each(jnp.add, plane_of(field, 0, k), each_fine(ahead, k)), k)


def hand_out_kernel(end_ref, next_ref, end_out, next_out, sems):
    copies = [
        pltpu.make_async_copy(end_ref, end_out, sems.at[0]),
        pltpu.make_async_copy(next_ref, next_out, sems.at[1]),
    ]
    for copy in copies:
        copy.start()
    for copy in copies:
        copy.wait()


def hand_out(end, following):
    return pl.pallas_call(
        hand_out_kernel,
        out_shape=[jax.ShapeDtypeStruct(end.shape, end.dtype)] * 2,
        in_specs=[pl.BlockSpec(memory_space=pltpu.VMEM)] * 2,
        out_specs=[pl.BlockSpec(memory_space=pl.ANY)] * 2,
        scratch_shapes=[pltpu.SemaphoreType.DMA((2,))],
    )(*(pltpu.with_memory_space_constraint(x, pltpu.VMEM) for x in (end, following)))


def solution(mesh):
    slabs, parts = mesh.shape["tm"], mesh.shape["gz"]

    def per_device(starts, cell_rates):
        depth, rows, lanes = cell_rates.shape
        layers = depth * parts
        groups = slabs // 2
        vectors = rows // SUBLANES
        fine = (vectors, SUBLANES, lanes)
        coarse = (vectors // 2, SUBLANES, lanes)
        packed = (layers // 4, *coarse)
        lead = (depth // 2, *coarse)
        aside = max(parts - 1, 1)
        dma = pltpu.SemaphoreType.DMA

        def vmem(*shape):
            return pltpu.VMEM(shape, jnp.float32)

        ends = pl.pallas_call(
            functools.partial(kernel, slabs, parts),
            out_shape=[pltpu.VMEM(starts.shape, jnp.float32)] * 2,
            in_specs=[pl.BlockSpec(memory_space=pl.ANY)] * 2,
            out_specs=[pl.BlockSpec(memory_space=pltpu.VMEM)] * 2,
            scratch_shapes=[
                vmem(2, layers, rows, lanes),
                vmem(layers, rows, lanes),
                vmem(layers, *fine),
                vmem(layers, *fine),
                vmem(2, 2, layers, *fine),
                vmem(2, layers, *fine),
                vmem(parts, 2, *packed),
                vmem(2, aside, *packed),
                vmem(groups, *packed),
                vmem(groups, parts, *packed),
                vmem(parts, *lead),
                vmem(parts, *lead),
                vmem(2, *lead),
                vmem(2, *lead),
                vmem(depth, *fine),
                vmem(aside, depth, *fine),
                vmem(*packed),
                vmem(layers, rows, lanes),
                pltpu.SemaphoreType.REGULAR((3,)),
                dma((9,)),
                dma((8 + groups,)),
            ],
            compiler_params=pltpu.CompilerParams(collective_id=0, has_side_effects=True),
        )(starts, cell_rates)
        return hand_out(*ends)

    return jax.shard_map(
        per_device,
        mesh=mesh,
        in_specs=(P("tm", "gz", None, None), P("gz", None, None)),
        out_specs=(P("tm", "gz", None, None), P("tm", "gz", None, None)),
        check_vma=False,
    )
```
